768 devices in a mesh: gx: 96 (over z_hi, x, y), gy: 8 (over z_lo, core).
Axes of the slice: x: 4, y: 8, z: 12 (z_hi: 3, z_lo: 4; z = z_hi * 4 + z_lo), core: 2. Of those that a mesh axis runs over, the one named last changes fastest.
Arguments:
- right_side: float32 [384, 512, 256], P('gx', 'gy'), may hold values from -40 to 40
- kappa_sq: float32 [384, 512, 256], P('gx', 'gy'), may hold values from 0.5 to 4
Outputs:
- solution_field: float32 [384, 512, 256], P('gx', 'gy')
- residual: float32 [384, 512, 256], P('gx', 'gy')
- residual_rms: float32 [3], replicated
The draws below stay inside these ranges and needn't reach their ends.
All inputs are finite; a program needn't handle non-finite values.
Results may differ from the reference program's by a relative error of at most 0.00016.
Values sent between devices are 32-bit elements; how exact they have to be, the bound alone decides.
No kernel may reach another device: no remote copies, remote signals or barrier semaphores. Data moves between devices by JAX's collectives and lax.ppermute only.
A program may use at most 32 MiB of HBM per device.

```python
import math
import jax
import jax.numpy as jnp

CZ = 256
ITERS = 3
NX = 384
NY = 512


def draw_right_side(key, part):
    first = jax.random.fold_in(key, 11)
    noise = jax.random.normal(first, (NX, NY, CZ), jnp.float32)
    place = jnp.arange(NX, dtype=jnp.float32) / NX
    rising = 1.0 + 2.0 * place
    values = noise * rising[:, None, None]
    return jnp.clip(values, -40.0, 40.0).astype(jnp.float32)


def level_of(key, shape, shards, least, largest):
    loudness = 1.0
    for axis_at, parts in shards:
        heights = jax.random.uniform(jax.random.fold_in(jax.random.fold_in(key, 6), axis_at), (parts,), jnp.float32, least / len(shards), largest / len(shards))
        loudness = loudness * jnp.repeat(jnp.exp(heights), shape[axis_at] // parts).reshape((-1,) + (1,) * (len(shape) - 1 - axis_at))
    return loudness


def setup_inputs(seed: int = 0) -> dict:
    key_of = jax.random.split(jax.random.key(seed), 3)
    return {
        "right_side": draw_right_side(jax.random.fold_in(key_of[2], 71), 0),
        "kappa_sq": jnp.clip(jnp.exp(math.log(4.0) - 2.0794415 * jax.random.uniform(key_of[1], (NX, NY, CZ), jnp.float32) ** level_of(key_of[1], (NX, NY, CZ), ((0, 96), (1, 8)), -0.2, 0.2)), 0.5, 4.0),
    }


def kpass(field, kappa_sq):
    beside = jnp.roll(field, 1, 0) + jnp.roll(field, -1, 0)
    beside = beside + jnp.roll(field, 1, 1) + jnp.roll(field, -1, 1)
    beside = beside + jnp.roll(field, 1, 2) + jnp.roll(field, -1, 2)
    return (6.0 + kappa_sq) * field - beside

def operate(field, kappa_sq):
    return kpass(kpass(field, kappa_sq), kappa_sq)

def reference(right_side, kappa_sq):
    shifted = 6.0 + kappa_sq
    precond = 1.0 / (shifted * shifted + 6.0)
    cells = right_side.shape[0] * right_side.shape[1] * right_side.shape[2]
    solution_field = jnp.zeros_like(right_side)
    residual = right_side
    u_vec = precond * residual
    w_vec = operate(u_vec, kappa_sq)
    p_vec = jnp.zeros_like(right_side)
    s_vec = jnp.zeros_like(right_side)
    q_vec = jnp.zeros_like(right_side)
    z_vec = jnp.zeros_like(right_side)
    norms = []
    gamma_old = jnp.float32(1.0)
    alpha_old = jnp.float32(1.0)
    for step in range(ITERS):
        gamma = jnp.sum(residual * u_vec)
        delta = jnp.sum(w_vec * u_vec)
        norm_sq = jnp.sum(residual * residual)
        norms.append(jnp.sqrt(norm_sq / cells))
        m_vec = precond * w_vec
        n_vec = operate(m_vec, kappa_sq)
        if step == 0:
            beta = jnp.float32(0.0)
            alpha = gamma / delta
        else:
            beta = gamma / gamma_old
            alpha = gamma / (delta - beta * gamma / alpha_old)
        z_vec = n_vec + beta * z_vec
        q_vec = m_vec + beta * q_vec
        s_vec = w_vec + beta * s_vec
        p_vec = u_vec + beta * p_vec
        solution_field = solution_field + alpha * p_vec
        residual = residual - alpha * s_vec
        u_vec = u_vec - alpha * q_vec
        w_vec = w_vec - alpha * z_vec
        gamma_old = gamma
        alpha_old = alpha
    return (solution_field, residual, jnp.stack(norms).astype(jnp.float32))
```

```python
import jax
import jax.numpy as jnp
from jax import lax
from jax.sharding import Mesh
from jax.sharding import PartitionSpec as P

ITERS = 3
GX = ("gx_0", "gx_1", "gx_2")
GY = ("gy_0", "gy_1")


def extended(x, sides, width):
    for axis, dim in sides:
        size, length = (lax.axis_size(axis), x.shape[dim])
        up = [(i, (i + 1) % size) for i in range(size)]
        down = [(j, i) for i, j in up]
        last = lax.slice_in_dim(x, length - width, length, axis=dim)
        first = lax.slice_in_dim(x, 0, width, axis=dim)
        before = lax.ppermute(last, axis, up)
        after = lax.ppermute(first, axis, down)
        x = jnp.concatenate([before, x, after], axis=dim)
    return x


def extended_2(x, sides, width):
    edges = {}
    for axis, dim in sides:
        size, length = (lax.axis_size(axis), x.shape[dim])
        up = [(i, (i + 1) % size) for i in range(size)]
        last = lax.slice_in_dim(x, length - width, length, axis=dim)
        first = lax.slice_in_dim(x, 0, width, axis=dim)
        edges[dim] = (
            lax.ppermute(last, axis, up),
            lax.ppermute(first, axis, [(b, a) for a, b in up]),
        )
    done = []
    for _, dim in sides:
        low, high = edges[dim]
        around = [(width, width) if d in done else (0, 0) for d in range(x.ndim)]
        x = jnp.concatenate([jnp.pad(low, around), x, jnp.pad(high, around)], axis=dim)
        done.append(dim)
    return x


def stage(x, axes):
    n = lax.axis_size(axes)
    return jnp.sum(lax.all_to_all(jnp.broadcast_to(x, (n, 1, 128)), axes, 0, 0), axis=0)


def totals(*sums):
    packed = jnp.pad(jnp.stack(sums), (0, 128 - len(sums))).reshape(1, 128)
    packed = stage(stage(packed, ("gx_1", "gx_2")), ("gx_0", "gy_0", "gy_1"))
    return [packed[0, i] for i in range(len(sums))]


def zbeside(field):
    return jnp.roll(field, 1, 2) + jnp.roll(field, -1, 2)


def operate_double(field, kappa_wide, kappa_sq):
    padded = extended(field, ((GX, 0), (GY, 1)), 2)
    center = padded[1:-1, 1:-1]
    beside = padded[2:, 1:-1] + padded[:-2, 1:-1]
    beside = beside + padded[1:-1, 2:] + padded[1:-1, :-2]
    beside = beside + zbeside(center)
    middle = (6.0 + kappa_wide) * center - beside
    inner = middle[1:-1, 1:-1]
    outer = middle[2:, 1:-1] + middle[:-2, 1:-1]
    outer = outer + middle[1:-1, 2:] + middle[1:-1, :-2]
    outer = outer + zbeside(inner)
    return (6.0 + kappa_sq) * inner - outer


def body(right_side, kappa_sq):
    shifted = 6.0 + kappa_sq
    precond = 1.0 / (shifted * shifted + 6.0)
    cells = (
        right_side.shape[0]
        * lax.axis_size(GX)
        * right_side.shape[1]
        * lax.axis_size(GY)
        * right_side.shape[2]
    )
    kappa_wide = extended_2(kappa_sq, ((GX, 0), (GY, 1)), 1)

    def operate(field):
        return operate_double(field, kappa_wide, kappa_sq)

    solution_field = jnp.zeros_like(right_side)
    residual = right_side
    u_vec = precond * residual
    w_vec = operate(u_vec)
    p_vec = jnp.zeros_like(right_side)
    s_vec = jnp.zeros_like(right_side)
    q_vec = jnp.zeros_like(right_side)
    z_vec = jnp.zeros_like(right_side)
    norms = []
    gamma_old = jnp.float32(1.0)
    alpha_old = jnp.float32(1.0)
    for step in range(ITERS):
        gamma, delta, norm_sq = totals(
            jnp.sum(residual * u_vec), jnp.sum(w_vec * u_vec), jnp.sum(residual * residual)
        )
        norms.append(jnp.sqrt(norm_sq / cells))
        m_vec = precond * w_vec
        n_vec = operate(m_vec)
        if step == 0:
            beta = jnp.float32(0.0)
            alpha = gamma / delta
        else:
            beta = gamma / gamma_old
            alpha = gamma / (delta - beta * gamma / alpha_old)
        z_vec = n_vec + beta * z_vec
        q_vec = m_vec + beta * q_vec
        s_vec = w_vec + beta * s_vec
        p_vec = u_vec + beta * p_vec
        solution_field = solution_field + alpha * p_vec
        residual = residual - alpha * s_vec
        u_vec = u_vec - alpha * q_vec
        w_vec = w_vec - alpha * z_vec
        gamma_old = gamma
        alpha_old = alpha
    return (solution_field, residual, jnp.stack(norms))


def solution(mesh):
    finer = Mesh(mesh.devices.reshape(3, 4, 8, 4, 2), ("gx_0", "gx_1", "gx_2", "gy_0", "gy_1"))
    in_specs = (P(GX, GY, None), P(GX, GY, None))
    out_specs = (P(GX, GY, None), P(GX, GY, None), P())
    return jax.shard_map(body, mesh=finer, in_specs=in_specs, out_specs=out_specs, check_vma=False)
```

```python
import functools

import jax
import jax.numpy as jnp
from jax import lax
from jax.experimental import pallas as pl
from jax.experimental.pallas import tpu as pltpu
from jax.sharding import Mesh
from jax.sharding import PartitionSpec as P

GX = ("gx_0", "gx_1", "gx_2")
GY = ("gy_0", "gy_1")
ALL = GX + GY
PLANE = ("gx_1", "gx_2")
COLUMN = ("gx_0", "gy_0", "gy_1")
HI, XS, YS, RANKS = 3, 4, 8, 8
NGX = HI * XS * YS
SEG = XS * YS
VMEM = pl.BlockSpec(memory_space=pltpu.VMEM)
F32 = jnp.float32


def over_gx(moves):
    return [(a % NGX * RANKS + h, b % NGX * RANKS + h) for a, b in moves for h in range(RANKS)]


def corner(hi, x, y):
    return hi % HI * SEG + x % XS * YS + y % YS


def FIRST(k):
    return corner(k, 0, 0)


def LAST(k):
    return corner(k, XS - 1, YS - 1)


def SIDE_A(k):
    return corner(k, 0, YS - 1)


def SIDE_B(k):
    return corner(k, XS - 1, 0)


SEGS = range(HI)
UP = over_gx([(g, g + 1) for g in range(NGX) if g % SEG != SEG - 1])
DOWN = over_gx([(g, g - 1) for g in range(NGX) if g % SEG])
UP2 = over_gx([(g, g + 2) for g in range(NGX)])
DOWN2 = over_gx([(g, g - 2) for g in range(NGX)])
ROUTES = [
    (
        over_gx([(LAST(k), SIDE_A(k)) for k in SEGS] + [(FIRST(k), SIDE_B(k)) for k in SEGS]),
        over_gx([(SIDE_A(k), FIRST(k + 1)) for k in SEGS] + [(SIDE_B(k), LAST(k - 1)) for k in SEGS]),
    ),
    (
        over_gx([(LAST(k), SIDE_B(k)) for k in SEGS] + [(FIRST(k), SIDE_A(k)) for k in SEGS]),
        over_gx([(SIDE_B(k), FIRST(k + 1)) for k in SEGS] + [(SIDE_A(k), LAST(k - 1)) for k in SEGS]),
    ),
    (
        over_gx([(LAST(k), FIRST(k)) for k in SEGS] + [(FIRST(k), LAST(k)) for k in SEGS]),
        over_gx([(FIRST(k), FIRST(k + 1)) for k in SEGS] + [(LAST(k), LAST(k - 1)) for k in SEGS]),
    ),
]
CUTS = ((0, 3), (3, 6), (6, 8))
GY_UP = [(g * RANKS + h, g * RANKS + (h + 1) % RANKS) for g in range(NGX) for h in range(RANKS)]
GY_DOWN = [(b, a) for a, b in GY_UP]

ORDER = (("v", 0), ("v", 1), ("k", 0), ("k", 1), ("k", 2), ("v", 2), ("v", 3), ("k", 3))
AT = {what: i for i, what in enumerate(ORDER)}
V_PLANES = (
    [("pp", 0), ("pp", 1)]
    + [("prev", AT["v", i]) for i in range(4)]
    + [("own", AT["v", i]) for i in range(4)]
    + [("next", AT["v", i]) for i in range(4)]
    + [("nn", 0), ("nn", 1)]
)
K_PLANES = (
    [("pp", 2)]
    + [("prev", AT["k", i]) for i in range(4)]
    + [("own", AT["k", i]) for i in range(4)]
    + [("next", AT["k", i]) for i in range(4)]
    + [("nn", 2)]
)
PARTS = ("pp", "prev", "own", "next", "nn")


def two_sum(a, b):
    s = a + b
    t = s - a
    return s, (a - (s - t)) + (b - t)


def quick(a, b):
    s = a + b
    return s, b - (s - a)


def halves(a):
    c = a * F32(4097.0)
    h = c - (c - a)
    return h, a - h


def two_prod(a, b):
    p = a * b
    (ah, al), (bh, bl) = halves(a), halves(b)
    return p, ((ah * bh - p) + ah * bl + al * bh) + al * bl


def add(a, b):
    s, e = two_sum(a[0], b[0])
    t, f = two_sum(a[1], b[1])
    s, e = quick(s, e + t)
    return quick(s, e + f)


def neg(a):
    return -a[0], -a[1]


def sub(a, b):
    return add(a, neg(b))


def mul(a, b):
    p, e = two_prod(a[0], b[0])
    return quick(p, e + (a[0] * b[1] + a[1] * b[0]))


def twice(a):
    return a[0] + a[0], a[1] + a[1]


def div(a, b):
    q = a[0] / b[0]
    r = sub(a, mul(b, (q, jnp.zeros_like(q))))
    return quick(q, r[0] / b[0])


def form(c, table):
    n = len(c)
    total = None
    for a in range(n):
        for b in range(a, n):
            t = table(a, b)
            for f in (c[a], c[b]):
                t = t if f is None else mul(t, f)
            t = t if a == b else twice(t)
            total = t if total is None else add(total, t)
    return total


def coefficients(mu, gram):
    hankel = lambda a, b: mu[a + b]
    lifted = lambda a, b: mu[a + b + 1]
    gamma = mu[0]
    alpha0 = div(gamma, mu[1])
    rr = [gram(0, 0)]
    r1 = [None, neg(alpha0)]
    gamma1 = form(r1, hankel)
    delta1 = form(r1, lifted)
    rr.append(form(r1, gram))
    beta1 = div(gamma1, gamma)
    alpha1 = div(gamma1, sub(delta1, div(mul(beta1, gamma1), alpha0)))
    one = (jnp.ones_like(alpha0[0]), jnp.zeros_like(alpha0[0]))
    p1 = [add(one, beta1), neg(alpha0)]
    step1 = [mul(alpha1, p1[0]), mul(alpha1, p1[1])]
    r2 = [None, sub(neg(alpha0), step1[0]), neg(step1[1])]
    gamma2 = form(r2, hankel)
    delta2 = form(r2, lifted)
    rr.append(form(r2, gram))
    beta2 = div(gamma2, gamma1)
    alpha2 = div(gamma2, sub(delta2, div(mul(beta2, gamma2), alpha1)))
    p2 = [add(one, mul(beta2, p1[0])), add(r2[1], mul(beta2, p1[1])), r2[2]]
    x = [
        add(add(alpha0, step1[0]), mul(alpha2, p2[0])),
        add(step1[1], mul(alpha2, p2[1])),
        mul(alpha2, p2[2]),
    ]
    return [c[0] for c in x], [c[0] for c in rr]


def around(src, i):
    c = src[i]
    rows, lanes = c.shape
    total = src[i - 1] + src[i + 1]
    total = total + pltpu.roll(c, 1, 0) + pltpu.roll(c, rows - 1, 0)
    return c, total + pltpu.roll(c, 1, 1) + pltpu.roll(c, lanes - 1, 1)


def lanes_of(shape):
    return lax.broadcasted_iota(jnp.int32, shape, len(shape) - 1)


def powers_kernel(
    rhs, pp, prev, own, nxt, nn, low, high,
    y1_out, y2_out, y3_out, sums_out,
    v, k, t1, w1, t2, w2, t3, y1s, y2s, rows,
):
    parts = dict(zip(PARTS, (pp, prev, own, nxt, nn)))
    for j, (name, at) in enumerate(V_PLANES):
        v[j, 8:72] = parts[name][at]
        v[j, 0:8] = low[j]
        v[j, 72:80] = high[j]
    for j, (name, at) in enumerate(K_PLANES):
        k[j, 8:72] = 6.0 + parts[name][at]
        k[j, 0:8] = 6.0 + low[16 + j]
        k[j, 72:80] = 6.0 + high[16 + j]

    def apply(src, dst, shift, count):
        @pl.loop(0, count)
        def _(i):
            c, near = around(src, i + 1)
            dst[i] = k[i + shift] * c - near

    def apply_scaled(src, plain, scaled, shift, count):
        @pl.loop(0, count)
        def _(i):
            c, near = around(src, i + 1)
            kk = k[i + shift]
            y = kk * c - near
            plain[i] = y
            scaled[i] = (1.0 / (kk * kk + 6.0)) * y

    apply(v, t1, 0, 14)
    apply_scaled(t1, y1s, w1, 1, 12)
    apply(w1, t2, 2, 10)
    apply_scaled(t2, y2s, w2, 3, 8)
    apply(w2, t3, 4, 6)

    def folded(a, b):
        prod = a * b
        prod = prod[:, :128] + prod[:, 128:]
        out = [prod[8 * j : 8 * j + 8] for j in range(8)]
        while len(out) > 1:
            out = [out[2 * j] + out[2 * j + 1] for j in range(len(out) // 2)]
        return out[0]

    rows[...] = jnp.zeros_like(rows)

    @pl.loop(0, 4)
    def _(i):
        c, near = around(t3, i + 1)
        y3_out[i] = (k[i + 5] * c - near)[8:72]
        y0 = rhs[i]
        y1 = y1s[i + 4, 8:72]
        y2 = y2s[i + 2, 8:72]
        y1_out[i] = y1
        y2_out[i] = y2
        v0, v1, v2, g = v[i + 6, 8:72], w1[i + 4, 8:72], w2[i + 2, 8:72], c[8:72]
        pairs = (
            (y0, v0), (y1, v0), (y1, v1), (y2, v1), (y2, v2), (g, g),
            (y0, y0), (y0, y1), (y0, y2), (y1, y1), (y1, y2), (y2, y2),
        )
        for d, (a, b) in enumerate(pairs):
            rows[8 * d : 8 * d + 8] += folded(a, b)

    terms = [(rows[pl.ds(s, 16, stride=8), :], None) for s in range(8)]
    hi, lo = terms[0][0], jnp.zeros((16, 128), F32)
    for s in range(1, 8):
        hi, e = two_sum(hi, terms[s][0])
        lo = lo + e
    for shift in (64, 32, 16, 8, 4, 2, 1):
        hi, e = two_sum(hi, pltpu.roll(hi, shift, 1))
        lo = lo + pltpu.roll(lo, shift, 1) + e
    row = lax.broadcasted_iota(jnp.int32, (16, 128), 0)
    lane = lanes_of((16, 128))
    packed = jnp.where(lane == row, hi, 0.0) + jnp.where(lane == row + 16, lo, 0.0)
    sums_out[...] = jnp.broadcast_to(jnp.sum(packed, axis=0, keepdims=True), sums_out.shape)


def added(parts):
    tiles = [parts[8 * j : 8 * j + 8] for j in range(parts.shape[0] // 8)]
    hi, lo = tiles[0], jnp.zeros((8, 128), F32)
    for tile in tiles[1:]:
        hi, e = two_sum(hi, tile)
        lo = lo + e
    for shift in (4, 2, 1):
        hi, e = two_sum(hi, pltpu.roll(hi, shift, 0))
        lo = lo + pltpu.roll(lo, shift, 0) + e
    lane = lanes_of((8, 128))
    return hi + jnp.where((lane >= 16) & (lane < 32), pltpu.roll(lo, 16, 1), 0.0)


def add_kernel(parts, out):
    out[...] = jnp.broadcast_to(added(parts[...])[0:1], out.shape)


def finish_kernel(cells, parts, rhs, kappa, y1, y2, y3, x_out, r_out, rms_out):
    total = added(parts[...])[0:1]
    lane = lanes_of((1, 128))

    def pair(d):
        take = lambda i: jnp.sum(jnp.where(lane == i, total, 0.0), axis=1, keepdims=True)
        return take(d), take(d + 16)

    mu = [pair(d) for d in range(6)]
    table = [pair(6 + d) for d in range(6)]
    place = {(0, 0): 0, (0, 1): 1, (0, 2): 2, (1, 1): 3, (1, 2): 4, (2, 2): 5}
    c, rr = coefficients(mu, lambda a, b: table[place[a, b]])
    rms = jnp.zeros((1, 128), F32)
    for i in range(3):
        rms = jnp.where(lane == i, jnp.sqrt(rr[i] / F32(cells)), rms)
    rms_out[...] = rms
    wide = [jnp.broadcast_to(a, rhs.shape[1:]) for a in c]

    @pl.loop(0, 4)
    def _(i):
        a0, a1, a2 = rhs[i], y1[i], y2[i]
        kk = 6.0 + kappa[i]
        x_out[i] = (1.0 / (kk * kk + 6.0)) * (wide[0] * a0 + wide[1] * a1 + wide[2] * a2)
        r_out[i] = a0 - (wide[0] * a1 + wide[1] * a2 + wide[2] * y3[i])


def kernel(fn, outs, scratch=(), flops=0):
    return pl.pallas_call(
        fn,
        out_shape=[jax.ShapeDtypeStruct(s, F32) for s in outs],
        scratch_shapes=[pltpu.VMEM(s, F32) for s in scratch],
        cost_estimate=pl.CostEstimate(flops=flops, bytes_accessed=flops // 8 + 1024, transcendentals=0),
    )


def send(x, pairs):
    return lax.ppermute(x, ALL, pairs)


def neighbours(block):
    relayed = [send(block[a:b], spread) for (a, b), (spread, _) in zip(CUTS, ROUTES)]
    up = send(block, UP)
    down = send(block, DOWN)
    pp = send(block[5:8], UP2)
    nn = send(block[0:3], DOWN2)
    far = jnp.concatenate([send(x, onward) for x, (_, onward) in zip(relayed, ROUTES)], axis=0)
    place = lax.axis_index(PLANE)
    prev = jnp.where(place == 0, far, up)
    nxt = jnp.where(place == SEG - 1, far, down)
    return pp, prev, nxt, nn


def body(right_side, kappa_sq):
    cells = right_side.size * NGX * RANKS
    shifted = 6.0 + kappa_sq
    start = (1.0 / (shifted * shifted + 6.0)) * right_side
    source = {"v": start, "k": kappa_sq}
    own = jnp.stack([source[a][i] for a, i in ORDER])
    pp, prev, nxt, nn = neighbours(own)
    parts = dict(zip(PARTS, (pp, prev, own, nxt, nn)))
    edge = lambda cut: jnp.stack([parts[name][at, cut] for name, at in V_PLANES + K_PLANES])
    low = send(edge(slice(56, 64)), GY_UP)
    high = send(edge(slice(0, 8)), GY_DOWN)
    block, wide = right_side.shape, (80, 256)
    n_plane, n_column = lax.axis_size(PLANE), lax.axis_size(COLUMN)
    counts = (16, 14, 14, 12, 10, 8, 6, 12, 8)
    y1, y2, y3, sums = kernel(
        powers_kernel,
        [block] * 3 + [(n_plane, 128)],
        [(n, *wide) for n in counts] + [(128, 128)],
        flops=20_000_000,
    )(right_side, pp, prev, own, nxt, nn, low, high)
    sums = lax.all_to_all(sums.reshape(n_plane, 1, 128), PLANE, 0, 0).reshape(n_plane, 128)
    (sums,) = kernel(add_kernel, [(n_column, 128)], flops=20000)(sums)
    sums = lax.all_to_all(sums.reshape(n_column, 1, 128), COLUMN, 0, 0).reshape(n_column, 128)
    x, r, rms = kernel(
        functools.partial(finish_kernel, cells), [block, block, (1, 128)], flops=2_000_000
    )(sums, right_side, kappa_sq, y1, y2, y3)
    return x, r, rms[0, :3]


def solution(mesh):
    finer = Mesh(mesh.devices.reshape(3, 4, 8, 4, 2), ("gx_0", "gx_1", "gx_2", "gy_0", "gy_1"))
    in_specs = (P(GX, GY, None), P(GX, GY, None))
    out_specs = (P(GX, GY, None), P(GX, GY, None), P())
    return jax.shard_map(body, mesh=finer, in_specs=in_specs, out_specs=out_specs, check_vma=False)
```

```python
import functools

import jax
import jax.numpy as jnp
from jax import lax
from jax.experimental import pallas as pl
from jax.experimental.pallas import tpu as pltpu
from jax.sharding import Mesh
from jax.sharding import PartitionSpec as P


GX = ("gx_0", "gx_1", "gx_2")
GY = ("gy_0", "gy_1")
ALL = GX + GY
PLANE = ("gx_1", "gx_2")
COLUMN = ("gx_0", "gy_0", "gy_1")
HI, XS, YS, RANKS = 3, 4, 8, 8
NGX = HI * XS * YS
SEG = XS * YS
VMEM = pl.BlockSpec(memory_space=pltpu.VMEM)
F32 = jnp.float32


def over_gx(moves):
    return [(a % NGX * RANKS + h, b % NGX * RANKS + h) for a, b in moves for h in range(RANKS)]


def corner(hi, x, y):
    return hi % HI * SEG + x % XS * YS + y % YS


def FIRST(k):
    return corner(k, 0, 0)


def LAST(k):
    return corner(k, XS - 1, YS - 1)


def SIDE_A(k):
    return corner(k, 0, YS - 1)


def SIDE_B(k):
    return corner(k, XS - 1, 0)


def NEAR_LAST(k):
    return corner(k, XS - 2, YS - 1)


def NEAR_FIRST(k):
    return corner(k, 1, 0)


SEGS = range(HI)
EVEN = over_gx([(g, g ^ 1) for g in range(NGX)])
ODD = over_gx([(g, ((g + 1) ^ 1) - 1) for g in range(NGX) if g % SEG not in (0, SEG - 1)])
STEP = over_gx(
    [(LAST(k), FIRST(k + 1)) for k in SEGS] + [(FIRST(k), LAST(k - 1)) for k in SEGS]
)
ACROSS = over_gx(
    [(LAST(k) - 1, FIRST(k + 1)) for k in SEGS] + [(FIRST(k) + 1, LAST(k - 1)) for k in SEGS]
)
ROUTES = [
    (
        over_gx([(LAST(k), SIDE_A(k)) for k in SEGS] + [(FIRST(k), SIDE_B(k)) for k in SEGS]),
        over_gx([(SIDE_A(k), FIRST(k + 1)) for k in SEGS] + [(SIDE_B(k), LAST(k - 1)) for k in SEGS]),
    ),
    (
        over_gx([(LAST(k), SIDE_B(k)) for k in SEGS] + [(FIRST(k), SIDE_A(k)) for k in SEGS]),
        over_gx([(SIDE_B(k), FIRST(k + 1)) for k in SEGS] + [(SIDE_A(k), LAST(k - 1)) for k in SEGS]),
    ),
    (
        over_gx([(LAST(k), NEAR_LAST(k)) for k in SEGS] + [(FIRST(k), NEAR_FIRST(k)) for k in SEGS]),
        over_gx([(NEAR_LAST(k), FIRST(k + 1)) for k in SEGS] + [(NEAR_FIRST(k), LAST(k - 1)) for k in SEGS]),
    ),
]
GY_UP = [(g * RANKS + h, g * RANKS + (h + 1) % RANKS) for g in range(NGX) for h in range(RANKS)]
GY_DOWN = [(b, a) for a, b in GY_UP]

ORDER = (("v", 0), ("v", 1), ("k", 0), ("k", 1), ("k", 2), ("v", 2), ("v", 3), ("k", 3))
AT = {what: i for i, what in enumerate(ORDER)}
PLANES = (
    [("pp", 0), ("pp", 1)]
    + [(name, AT["v", i]) for name in ("prev", "own", "next") for i in range(4)]
    + [("nn", 0), ("nn", 1), ("pp", 2)]
    + [(name, AT["k", i]) for name in ("prev", "own", "next") for i in range(4)]
    + [("nn", 2)]
)


def two_sum(a, b):
    s = a + b
    t = s - a
    return s, (a - (s - t)) + (b - t)


def quick(a, b):
    s = a + b
    return s, b - (s - a)


def halves(a):
    c = a * F32(4097.0)
    h = c - (c - a)
    return h, a - h


def two_prod(a, b):
    p = a * b
    (ah, al), (bh, bl) = halves(a), halves(b)
    return p, ((ah * bh - p) + ah * bl + al * bh) + al * bl


def add(a, b):
    s, e = two_sum(a[0], b[0])
    t, f = two_sum(a[1], b[1])
    s, e = quick(s, e + t)
    return quick(s, e + f)


def neg(a):
    return -a[0], -a[1]


def sub(a, b):
    return add(a, neg(b))


def mul(a, b):
    p, e = two_prod(a[0], b[0])
    return quick(p, e + (a[0] * b[1] + a[1] * b[0]))


def twice(a):
    return a[0] + a[0], a[1] + a[1]


def div(a, b):
    q = a[0] / b[0]
    r = sub(a, mul(b, (q, jnp.zeros_like(q))))
    return quick(q, r[0] / b[0])


def form(c, table):
    n = len(c)
    total = None
    for a in range(n):
        for b in range(a, n):
            t = table(a, b)
            for f in (c[a], c[b]):
                t = t if f is None else mul(t, f)
            t = t if a == b else twice(t)
            total = t if total is None else add(total, t)
    return total


def coefficients(mu, gram):
    hankel = lambda a, b: mu[a + b]
    lifted = lambda a, b: mu[a + b + 1]
    gamma = mu[0]
    alpha0 = div(gamma, mu[1])
    rr = [gram(0, 0)]
    r1 = [None, neg(alpha0)]
    gamma1 = form(r1, hankel)
    delta1 = form(r1, lifted)
    rr.append(form(r1, gram))
    beta1 = div(gamma1, gamma)
    alpha1 = div(gamma1, sub(delta1, div(mul(beta1, gamma1), alpha0)))
    one = (jnp.ones_like(alpha0[0]), jnp.zeros_like(alpha0[0]))
    p1 = [add(one, beta1), neg(alpha0)]
    step1 = [mul(alpha1, p1[0]), mul(alpha1, p1[1])]
    r2 = [None, sub(neg(alpha0), step1[0]), neg(step1[1])]
    gamma2 = form(r2, hankel)
    delta2 = form(r2, lifted)
    rr.append(form(r2, gram))
    beta2 = div(gamma2, gamma1)
    alpha2 = div(gamma2, sub(delta2, div(mul(beta2, gamma2), alpha1)))
    p2 = [add(one, mul(beta2, p1[0])), add(r2[1], mul(beta2, p1[1])), r2[2]]
    x = [
        add(add(alpha0, step1[0]), mul(alpha2, p2[0])),
        add(step1[1], mul(alpha2, p2[1])),
        mul(alpha2, p2[2]),
    ]
    return [c[0] for c in x], [c[0] for c in rr]


def around(src, i):
    c = src[i]
    rows, lanes = c.shape
    total = src[i - 1] + src[i + 1]
    total = total + pltpu.roll(c, 1, 0) + pltpu.roll(c, rows - 1, 0)
    return c, total + pltpu.roll(c, 1, 1) + pltpu.roll(c, lanes - 1, 1)


def lanes_of(shape):
    return lax.broadcasted_iota(jnp.int32, shape, len(shape) - 1)


def is_odd():
    return lax.rem(lax.axis_index("gx_2"), 2) == 1


def at_step():
    place = lax.axis_index("gx_1") * YS + lax.axis_index("gx_2")
    return (place == 0) | (place == SEG - 1)


def start_kernel(flags, rhs, kappa, own, p0, p1, p2, p3, across):
    for i in range(4):
        k = kappa[i]
        shifted = 6.0 + k
        own[AT["v", i]] = (1.0 / (shifted * shifted + 6.0)) * rhs[i]
        own[AT["k", i]] = k
    for i, piece in enumerate((p0, p1, p2, p3)):
        piece[...] = own[2 * i : 2 * i + 2]

    @pl.when(flags[0] == 1)
    def _():
        across[...] = own[0:3]

    @pl.when(flags[0] == 0)
    def _():
        across[...] = own[5:8]


def forward_odd_kernel(flags, even, out):
    @pl.when(flags[0] == 1)
    def _():
        out[...] = even[5:8]

    @pl.when(flags[0] == 0)
    def _():
        out[...] = even[0:3]


def forward_even_kernel(flags, odd, d0, d1, d2, d3, out, block):
    @pl.when(flags[1] == 0)
    def _():
        block[...] = odd[...]

    @pl.when(flags[1] == 1)
    def _():
        for i, piece in enumerate((d0, d1, d2, d3)):
            block[2 * i : 2 * i + 2] = piece[...]

    @pl.when(flags[0] == 1)
    def _():
        out[...] = block[0:3]

    @pl.when(flags[0] == 0)
    def _():
        out[...] = block[5:8]


def gather_kernel(flags, own, even, odd, even2, odd2, across, center, first, last):
    def lay(names):
        for j, (name, at) in enumerate(PLANES):
            if name in names:
                plane = names[name][at]
                center[j] = plane
                first[j] = plane[0:8]
                last[j] = plane[56:64]

    lay({"own": own})
    odd_place = flags[0] == 1
    inner = flags[1] == 0

    @pl.when(odd_place)
    def _():
        lay({"prev": even, "next": odd, "pp": even2})

    @pl.when(odd_place & inner)
    def _():
        lay({"nn": odd2})

    @pl.when(odd_place & ~inner)
    def _():
        lay({"nn": across})

    @pl.when(~odd_place)
    def _():
        lay({"prev": odd, "next": even, "nn": even2})

    @pl.when(~odd_place & inner)
    def _():
        lay({"pp": odd2})

    @pl.when(~odd_place & ~inner)
    def _():
        lay({"pp": across})


def powers_kernel(
    rhs, center, low, high,
    y1_out, y2_out, y3_out, sums_out,
    v, k, t1, w1, t2, w2, t3, y1s, y2s, rows,
):
    for j in range(16):
        v[j, 8:72] = center[j]
        v[j, 0:8] = low[j]
        v[j, 72:80] = high[j]
    for j in range(14):
        k[j, 8:72] = 6.0 + center[16 + j]
        k[j, 0:8] = 6.0 + low[16 + j]
        k[j, 72:80] = 6.0 + high[16 + j]

    def apply(src, dst, shift, count):
        @pl.loop(0, count)
        def _(i):
            c, near = around(src, i + 1)
            dst[i] = k[i + shift] * c - near

    def apply_scaled(src, plain, scaled, shift, count):
        @pl.loop(0, count)
        def _(i):
            c, near = around(src, i + 1)
            kk = k[i + shift]
            y = kk * c - near
            plain[i] = y
            scaled[i] = (1.0 / (kk * kk + 6.0)) * y

    apply(v, t1, 0, 14)
    apply_scaled(t1, y1s, w1, 1, 12)
    apply(w1, t2, 2, 10)
    apply_scaled(t2, y2s, w2, 3, 8)
    apply(w2, t3, 4, 6)

    def folded(a, b):
        prod = a * b
        prod = prod[:, :128] + prod[:, 128:]
        out = [prod[8 * j : 8 * j + 8] for j in range(8)]
        while len(out) > 1:
            out = [out[2 * j] + out[2 * j + 1] for j in range(len(out) // 2)]
        return out[0]

    rows[...] = jnp.zeros_like(rows)

    @pl.loop(0, 4)
    def _(i):
        c, near = around(t3, i + 1)
        y3_out[i] = (k[i + 5] * c - near)[8:72]
        y0 = rhs[i]
        y1 = y1s[i + 4, 8:72]
        y2 = y2s[i + 2, 8:72]
        y1_out[i] = y1
        y2_out[i] = y2
        v0, v1, v2, g = v[i + 6, 8:72], w1[i + 4, 8:72], w2[i + 2, 8:72], c[8:72]
        pairs = (
            (y0, v0), (y1, v0), (y1, v1), (y2, v1), (y2, v2), (g, g),
            (y0, y0), (y0, y1), (y0, y2), (y1, y1), (y1, y2), (y2, y2),
        )
        for d, (a, b) in enumerate(pairs):
            rows[8 * d : 8 * d + 8] += folded(a, b)

    terms = [(rows[pl.ds(s, 16, stride=8), :], None) for s in range(8)]
    hi, lo = terms[0][0], jnp.zeros((16, 128), F32)
    for s in range(1, 8):
        hi, e = two_sum(hi, terms[s][0])
        lo = lo + e
    for shift in (64, 32, 16, 8, 4, 2, 1):
        hi, e = two_sum(hi, pltpu.roll(hi, shift, 1))
        lo = lo + pltpu.roll(lo, shift, 1) + e
    row = lax.broadcasted_iota(jnp.int32, (16, 128), 0)
    lane = lanes_of((16, 128))
    packed = jnp.where(lane == row, hi, 0.0) + jnp.where(lane == row + 16, lo, 0.0)
    sums_out[...] = jnp.broadcast_to(jnp.sum(packed, axis=0, keepdims=True), sums_out.shape)


def added(parts):
    tiles = [parts[8 * j : 8 * j + 8] for j in range(parts.shape[0] // 8)]
    hi, lo = tiles[0], jnp.zeros((8, 128), F32)
    for tile in tiles[1:]:
        hi, e = two_sum(hi, tile)
        lo = lo + e
    for shift in (4, 2, 1):
        hi, e = two_sum(hi, pltpu.roll(hi, shift, 0))
        lo = lo + pltpu.roll(lo, shift, 0) + e
    lane = lanes_of((8, 128))
    return hi + jnp.where((lane >= 16) & (lane < 32), pltpu.roll(lo, 16, 1), 0.0)


def add_kernel(parts, out):
    out[...] = jnp.broadcast_to(added(parts[...])[0:1], out.shape)


def finish_kernel(cells, parts, rhs, kappa, y1, y2, y3, x_out, r_out, rms_out):
    total = added(parts[...])[0:1]
    lane = lanes_of((1, 128))

    def pair(d):
        take = lambda i: jnp.sum(jnp.where(lane == i, total, 0.0), axis=1, keepdims=True)
        return take(d), take(d + 16)

    mu = [pair(d) for d in range(6)]
    table = [pair(6 + d) for d in range(6)]
    place = {(0, 0): 0, (0, 1): 1, (0, 2): 2, (1, 1): 3, (1, 2): 4, (2, 2): 5}
    c, rr = coefficients(mu, lambda a, b: table[place[a, b]])
    for i in range(3):
        rms_out[i] = jnp.sqrt(rr[i] / F32(cells))[0, 0]
    wide = [jnp.broadcast_to(a, rhs.shape[1:]) for a in c]

    @pl.loop(0, 4)
    def _(i):
        a0, a1, a2 = rhs[i], y1[i], y2[i]
        kk = 6.0 + kappa[i]
        x_out[i] = (1.0 / (kk * kk + 6.0)) * (wide[0] * a0 + wide[1] * a1 + wide[2] * a2)
        r_out[i] = a0 - (wide[0] * a1 + wide[1] * a2 + wide[2] * y3[i])


def kernel(fn, outs, scratch=(), flops=0, flagged=False, scalars=False, limit=24):
    def call(*args):
        specs = [VMEM] * len(args)
        out_specs = [VMEM] * len(outs)
        if flagged:
            specs[0] = pl.BlockSpec(memory_space=pltpu.SMEM)
        if scalars:
            out_specs[-1] = pl.BlockSpec(memory_space=pltpu.SMEM)
        return pl.pallas_call(
            fn,
            out_shape=[jax.ShapeDtypeStruct(s, F32) for s in outs],
            in_specs=specs,
            out_specs=out_specs,
            scratch_shapes=[pltpu.VMEM(s, F32) for s in scratch],
            cost_estimate=pl.CostEstimate(
                flops=flops, bytes_accessed=flops // 8 + 1024, transcendentals=0
            ),
            compiler_params=pltpu.CompilerParams(vmem_limit_bytes=limit << 20),
        )(*args)

    return call


def send(x, pairs):
    return lax.ppermute(x, ALL, pairs)


def extended(flags, right_side, kappa_sq):
    _, cols, lanes = right_side.shape
    shape = lambda n: (n, cols, lanes)
    own, p0, p1, p2, p3, near = kernel(
        start_kernel, [shape(8)] + [shape(2)] * 4 + [shape(3)], flops=10**6, flagged=True
    )(flags, right_side, kappa_sq)
    relayed = [send(piece, spread) for piece, (spread, _) in zip((p0, p1, p2), ROUTES)]
    across = send(near, ACROSS)
    even = send(own, EVEN)
    odd = send(own, ODD)
    pieces = [send(x, onward) for x, (_, onward) in zip(relayed, ROUTES)]
    pieces.append(send(p3, STEP))
    (near,) = kernel(forward_odd_kernel, [shape(3)], flops=10**5, flagged=True)(flags, even)
    odd2 = send(near, ODD)
    near, odd = kernel(
        forward_even_kernel, [shape(3), shape(8)], flops=10**5, flagged=True
    )(flags, odd, *pieces)
    even2 = send(near, EVEN)
    edge = (len(PLANES), 8, lanes)
    return kernel(
        gather_kernel, [shape(len(PLANES)), edge, edge], flops=10**6, flagged=True
    )(flags, own, even, odd, even2, odd2, across)


def steps(right_side, kappa_sq):
    cells = right_side.size * NGX * RANKS
    flags = jnp.stack([is_odd(), at_step()]).astype(jnp.int32)
    center, first, last = extended(flags, right_side, kappa_sq)
    low = send(last, GY_UP)
    high = send(first, GY_DOWN)
    block, wide = right_side.shape, (80, 256)
    n_plane, n_column = lax.axis_size(PLANE), lax.axis_size(COLUMN)
    counts = (16, 14, 14, 12, 10, 8, 6, 12, 8)
    y1, y2, y3, sums = kernel(
        powers_kernel,
        [block] * 3 + [(n_plane, 128)],
        [(n, *wide) for n in counts] + [(128, 128)],
        flops=20_000_000,
    )(right_side, center, low, high)
    sums = lax.all_to_all(sums.reshape(n_plane, 1, 128), PLANE, 0, 0).reshape(n_plane, 128)
    (sums,) = kernel(add_kernel, [(n_column, 128)], flops=20000)(sums)
    sums = lax.all_to_all(sums.reshape(n_column, 1, 128), COLUMN, 0, 0).reshape(n_column, 128)
    return kernel(
        functools.partial(finish_kernel, cells), [block, block, (3,)], flops=2_000_000, scalars=True
    )(sums, right_side, kappa_sq, y1, y2, y3)


def solution(mesh):
    finer = Mesh(mesh.devices.reshape(3, 4, 8, 4, 2), ("gx_0", "gx_1", "gx_2", "gy_0", "gy_1"))
    in_specs = (P(GX, GY, None), P(GX, GY, None))
    out_specs = (P(GX, GY, None), P(GX, GY, None), P())
    return jax.shard_map(steps, mesh=finer, in_specs=in_specs, out_specs=out_specs, check_vma=False)
```

```python
import functools

import jax
import jax.numpy as jnp
from jax import lax
from jax.experimental import pallas as pl
from jax.experimental.pallas import tpu as pltpu
from jax.sharding import Mesh
from jax.sharding import PartitionSpec as P


GX = ("gx_0", "gx_1", "gx_2")
GY = ("gy_0", "gy_1")
ALL = GX + GY
PLANE = ("gx_1", "gx_2")
COLUMN = ("gx_0", "gy_0", "gy_1")
HI, XS, YS, RANKS = 3, 4, 8, 8
NGX = HI * XS * YS
SEG = XS * YS
VMEM = pl.BlockSpec(memory_space=pltpu.VMEM)
F32 = jnp.float32


def over_gx(moves):
    return [(a % NGX * RANKS + h, b % NGX * RANKS + h) for a, b in moves for h in range(RANKS)]


def corner(hi, x, y):
    return hi % HI * SEG + x % XS * YS + y % YS


def FIRST(k):
    return corner(k, 0, 0)


def LAST(k):
    return corner(k, XS - 1, YS - 1)


def SIDE_A(k):
    return corner(k, 0, YS - 1)


def SIDE_B(k):
    return corner(k, XS - 1, 0)


def NEAR_LAST(k):
    return corner(k, XS - 2, YS - 1)


def NEAR_FIRST(k):
    return corner(k, 1, 0)


SEGS = range(HI)
EVEN = over_gx([(g, g ^ 1) for g in range(NGX)])
ODD = over_gx([(g, ((g + 1) ^ 1) - 1) for g in range(NGX) if g % SEG not in (0, SEG - 1)])
STEP = over_gx(
    [(LAST(k), FIRST(k + 1)) for k in SEGS] + [(FIRST(k), LAST(k - 1)) for k in SEGS]
)
LOW2 = over_gx([(g, g ^ 2) for g in range(NGX)])
HIGH2 = over_gx([(g, ((g + 2) ^ 2) - 2) for g in range(NGX) if 1 < g % SEG < SEG - 2])
ACROSS = over_gx(
    [(LAST(k) - 1, FIRST(k + 1)) for k in SEGS] + [(FIRST(k) + 1, LAST(k - 1)) for k in SEGS]
)
ROUTES = [
    (
        over_gx([(LAST(k), SIDE_A(k)) for k in SEGS] + [(FIRST(k), SIDE_B(k)) for k in SEGS]),
        over_gx([(SIDE_A(k), FIRST(k + 1)) for k in SEGS] + [(SIDE_B(k), LAST(k - 1)) for k in SEGS]),
    ),
    (
        over_gx([(LAST(k), SIDE_B(k)) for k in SEGS] + [(FIRST(k), SIDE_A(k)) for k in SEGS]),
        over_gx([(SIDE_B(k), FIRST(k + 1)) for k in SEGS] + [(SIDE_A(k), LAST(k - 1)) for k in SEGS]),
    ),
    (
        over_gx([(LAST(k), NEAR_LAST(k)) for k in SEGS] + [(FIRST(k), NEAR_FIRST(k)) for k in SEGS]),
        over_gx([(NEAR_LAST(k), FIRST(k + 1)) for k in SEGS] + [(NEAR_FIRST(k), LAST(k - 1)) for k in SEGS]),
    ),
    (
        over_gx([(LAST(k), corner(k, XS - 1, 1)) for k in SEGS] + [(FIRST(k), corner(k, 0, YS - 2)) for k in SEGS]),
        over_gx(
            [(corner(k, XS - 1, 1), FIRST(k + 1) + 1) for k in SEGS]
            + [(corner(k, 0, YS - 2), LAST(k - 1) - 1) for k in SEGS]
        ),
    ),
]
GY_EVEN = [(g * RANKS + h, g * RANKS + (h ^ 1)) for g in range(NGX) for h in range(RANKS)]
GY_ODD = [
    (g * RANKS + h, g * RANKS + (((h + 1) ^ 1) - 1) % RANKS) for g in range(NGX) for h in range(RANKS)
]

ORDER = (("v", 0), ("v", 1), ("k", 0), ("k", 1), ("k", 2), ("v", 2), ("v", 3), ("k", 3))
AT = {what: i for i, what in enumerate(ORDER)}
PLANES = (
    [("pp", 0), ("pp", 1)]
    + [(name, AT["v", i]) for name in ("prev", "own", "next") for i in range(4)]
    + [("nn", 0), ("nn", 1), ("pp", 2)]
    + [(name, AT["k", i]) for name in ("prev", "own", "next") for i in range(4)]
    + [("nn", 2)]
)

WIDE = tuple(j for j in range(len(PLANES)) if j not in (0, 15, 16, 29))


def two_sum(a, b):
    s = a + b
    t = s - a
    return s, (a - (s - t)) + (b - t)


def quick(a, b):
    s = a + b
    return s, b - (s - a)


def halves(a):
    c = a * F32(4097.0)
    h = c - (c - a)
    return h, a - h


def two_prod(a, b):
    p = a * b
    (ah, al), (bh, bl) = halves(a), halves(b)
    return p, ((ah * bh - p) + ah * bl + al * bh) + al * bl


def add(a, b):
    s, e = two_sum(a[0], b[0])
    t, f = two_sum(a[1], b[1])
    s, e = quick(s, e + t)
    return quick(s, e + f)


def neg(a):
    return -a[0], -a[1]


def sub(a, b):
    return add(a, neg(b))


def mul(a, b):
    p, e = two_prod(a[0], b[0])
    return quick(p, e + (a[0] * b[1] + a[1] * b[0]))


def twice(a):
    return a[0] + a[0], a[1] + a[1]


def div(a, b):
    q = a[0] / b[0]
    r = sub(a, mul(b, (q, jnp.zeros_like(q))))
    return quick(q, r[0] / b[0])


def form(c, table):
    n = len(c)
    total = None
    for a in range(n):
        for b in range(a, n):
            t = table(a, b)
            for f in (c[a], c[b]):
                t = t if f is None else mul(t, f)
            t = t if a == b else twice(t)
            total = t if total is None else add(total, t)
    return total


def coefficients(mu, gram):
    hankel = lambda a, b: mu[a + b]
    lifted = lambda a, b: mu[a + b + 1]
    gamma = mu[0]
    alpha0 = div(gamma, mu[1])
    rr = [gram(0, 0)]
    r1 = [None, neg(alpha0)]
    gamma1 = form(r1, hankel)
    delta1 = form(r1, lifted)
    rr.append(form(r1, gram))
    beta1 = div(gamma1, gamma)
    alpha1 = div(gamma1, sub(delta1, div(mul(beta1, gamma1), alpha0)))
    one = (jnp.ones_like(alpha0[0]), jnp.zeros_like(alpha0[0]))
    p1 = [add(one, beta1), neg(alpha0)]
    step1 = [mul(alpha1, p1[0]), mul(alpha1, p1[1])]
    r2 = [None, sub(neg(alpha0), step1[0]), neg(step1[1])]
    gamma2 = form(r2, hankel)
    delta2 = form(r2, lifted)
    rr.append(form(r2, gram))
    beta2 = div(gamma2, gamma1)
    alpha2 = div(gamma2, sub(delta2, div(mul(beta2, gamma2), alpha1)))
    p2 = [add(one, mul(beta2, p1[0])), add(r2[1], mul(beta2, p1[1])), r2[2]]
    x = [
        add(add(alpha0, step1[0]), mul(alpha2, p2[0])),
        add(step1[1], mul(alpha2, p2[1])),
        mul(alpha2, p2[2]),
    ]
    return [c[0] for c in x], [c[0] for c in rr]


def around(src, i):
    c = src[i]
    rows, lanes = c.shape
    total = src[i - 1] + src[i + 1]
    total = total + pltpu.roll(c, 1, 0) + pltpu.roll(c, rows - 1, 0)
    return c, total + pltpu.roll(c, 1, 1) + pltpu.roll(c, lanes - 1, 1)


def lanes_of(shape):
    return lax.broadcasted_iota(jnp.int32, shape, len(shape) - 1)


def place_flags():
    place = lax.axis_index(PLANE)
    beside = (place == 0) | (place == SEG - 1)
    near = (place < 2) | (place >= SEG - 2)
    return jnp.stack(
        [place % 2 == 1, place % 4 >= 2, lax.axis_index("gy_1") == 1, beside, near]
    ).astype(jnp.int32)


def start_kernel(flags, rhs_hbm, kappa_hbm, own, p0, p1, p2, p3, low2, high2, rhs, kappa, sems):
    fetch = [
        pltpu.make_async_copy(rhs_hbm, rhs, sems.at[0]),
        pltpu.make_async_copy(kappa_hbm, kappa, sems.at[1]),
    ]
    for copy in fetch:
        copy.start()
    for copy in fetch:
        copy.wait()
    for i in range(4):
        k = kappa[i]
        shifted = 6.0 + k
        own[AT["v", i]] = (1.0 / (shifted * shifted + 6.0)) * rhs[i]
        own[AT["k", i]] = k
    for i, piece in enumerate((p0, p1, p2, p3)):
        piece[...] = own[2 * i : 2 * i + 2]

    @pl.when(flags[1] == 0)
    def _():
        low2[...] = own[5:8]
        high2[...] = own[0:3]

    @pl.when(flags[1] == 1)
    def _():
        low2[...] = own[0:3]
        high2[...] = own[5:8]


def gather_kernel(
    flags, own, even, odd, low2, high2, across, ahead, d0, d1, d2, d3, center, to_even, to_odd
):
    even_side = pl.multiple_of((1 - flags[2]) * 56, 8)
    odd_side = pl.multiple_of(flags[2] * 56, 8)

    def lay(part, ref):
        for j, (name, at) in enumerate(PLANES):
            if name == part:
                src, i = ((d0, d1, d2, d3)[at // 2], at % 2) if ref is None else (ref, at)
                center[j] = src[i]
                if j in WIDE:
                    to_even[WIDE.index(j)] = src[i, pl.ds(even_side, 8)]
                    to_odd[WIDE.index(j)] = src[i, pl.ds(odd_side, 8)]

    def when(*conditions):
        here = functools.reduce(lambda a, b: a & b, [flags[i] == value for i, value in conditions])
        return pl.when(here)

    lay("own", own)
    for value, (by_even, by_odd) in enumerate((("next", "prev"), ("prev", "next"))):

        @when((0, value))
        def _():
            lay(by_even, even)

        @when((0, value), (3, 0))
        def _():
            lay(by_odd, odd)

        @when((0, value), (3, 1))
        def _():
            lay(by_odd, None)

    for value, (by_low, by_high) in enumerate((("nn", "pp"), ("pp", "nn"))):

        @when((1, value))
        def _():
            lay(by_low, low2)

        @when((1, value), (4, 0))
        def _():
            lay(by_high, high2)

        @when((1, value), (3, 1))
        def _():
            lay(by_high, across)

        @when((1, value), (3, 0), (4, 1))
        def _():
            lay(by_high, ahead)


def powers_kernel(
    flags, rhs, center, even, odd,
    y1_out, y2_out, y3_out, sums_out,
    v, k, t1, w1, t2, w2, t3, y1s, y2s, rows,
):
    even_side = pl.multiple_of((1 - flags[2]) * 72, 8)
    odd_side = pl.multiple_of(flags[2] * 72, 8)
    for j in range(30):
        ref, at, base = (v, j, 0.0) if j < 16 else (k, j - 16, 6.0)
        put = lambda plane: plane if ref is v else base + plane
        ref[at, 8:72] = put(center[j])
        if j in WIDE:
            ref[at, pl.ds(even_side, 8)] = put(even[WIDE.index(j)])
            ref[at, pl.ds(odd_side, 8)] = put(odd[WIDE.index(j)])
        else:
            ref[at, 0:8] = jnp.zeros((8, ref.shape[2]), F32)
            ref[at, 72:80] = jnp.zeros((8, ref.shape[2]), F32)

    def apply(src, dst, shift, count):
        @pl.loop(0, count)
        def _(i):
            c, near = around(src, i + 1)
            dst[i] = k[i + shift] * c - near

    def apply_scaled(src, plain, scaled, shift, count):
        @pl.loop(0, count)
        def _(i):
            c, near = around(src, i + 1)
            kk = k[i + shift]
            y = kk * c - near
            plain[i] = y
            scaled[i] = (1.0 / (kk * kk + 6.0)) * y

    apply(v, t1, 0, 14)
    apply_scaled(t1, y1s, w1, 1, 12)
    apply(w1, t2, 2, 10)
    apply_scaled(t2, y2s, w2, 3, 8)
    apply(w2, t3, 4, 6)

    def folded(a, b):
        prod = a * b
        prod = prod[:, :128] + prod[:, 128:]
        out = [prod[8 * j : 8 * j + 8] for j in range(8)]
        while len(out) > 1:
            out = [out[2 * j] + out[2 * j + 1] for j in range(len(out) // 2)]
        return out[0]

    rows[...] = jnp.zeros_like(rows)

    @pl.loop(0, 4)
    def _(i):
        c, near = around(t3, i + 1)
        y3_out[i] = (k[i + 5] * c - near)[8:72]
        y0 = rhs[i]
        y1 = y1s[i + 4, 8:72]
        y2 = y2s[i + 2, 8:72]
        y1_out[i] = y1
        y2_out[i] = y2
        v0, v1, v2, g = v[i + 6, 8:72], w1[i + 4, 8:72], w2[i + 2, 8:72], c[8:72]
        pairs = (
            (y0, v0), (y1, v0), (y1, v1), (y2, v1), (y2, v2), (g, g),
            (y0, y0), (y0, y1), (y0, y2), (y1, y1), (y1, y2), (y2, y2),
        )
        for d, (a, b) in enumerate(pairs):
            rows[8 * d : 8 * d + 8] += folded(a, b)

    terms = [(rows[pl.ds(s, 16, stride=8), :], None) for s in range(8)]
    hi, lo = terms[0][0], jnp.zeros((16, 128), F32)
    for s in range(1, 8):
        hi, e = two_sum(hi, terms[s][0])
        lo = lo + e
    for shift in (64, 32, 16, 8, 4, 2, 1):
        hi, e = two_sum(hi, pltpu.roll(hi, shift, 1))
        lo = lo + pltpu.roll(lo, shift, 1) + e
    row = lax.broadcasted_iota(jnp.int32, (16, 128), 0)
    lane = lanes_of((16, 128))
    packed = jnp.where(lane == row, hi, 0.0) + jnp.where(lane == row + 16, lo, 0.0)
    sums_out[...] = jnp.broadcast_to(jnp.sum(packed, axis=0, keepdims=True), sums_out.shape)


def added(parts):
    tiles = [parts[8 * j : 8 * j + 8] for j in range(parts.shape[0] // 8)]
    hi, lo = tiles[0], jnp.zeros((8, 128), F32)
    for tile in tiles[1:]:
        hi, e = two_sum(hi, tile)
        lo = lo + e
    for shift in (4, 2, 1):
        hi, e = two_sum(hi, pltpu.roll(hi, shift, 0))
        lo = lo + pltpu.roll(lo, shift, 0) + e
    lane = lanes_of((8, 128))
    return hi + jnp.where((lane >= 16) & (lane < 32), pltpu.roll(lo, 16, 1), 0.0)


def add_kernel(parts, out):
    out[...] = jnp.broadcast_to(added(parts[...])[0:1], out.shape)


def finish_kernel(cells, parts, rhs, kappa, y1, y2, y3, x_out, r_out, rms_out):
    total = added(parts[...])[0:1]
    lane = lanes_of((1, 128))

    def pair(d):
        take = lambda i: jnp.sum(jnp.where(lane == i, total, 0.0), axis=1, keepdims=True)
        return take(d), take(d + 16)

    mu = [pair(d) for d in range(6)]
    table = [pair(6 + d) for d in range(6)]
    place = {(0, 0): 0, (0, 1): 1, (0, 2): 2, (1, 1): 3, (1, 2): 4, (2, 2): 5}
    c, rr = coefficients(mu, lambda a, b: table[place[a, b]])
    for i in range(3):
        rms_out[i] = jnp.sqrt(rr[i] / F32(cells))[0, 0]
    wide = [jnp.broadcast_to(a, rhs.shape[1:]) for a in c]

    @pl.loop(0, 4)
    def _(i):
        a0, a1, a2 = rhs[i], y1[i], y2[i]
        kk = 6.0 + kappa[i]
        x_out[i] = (1.0 / (kk * kk + 6.0)) * (wide[0] * a0 + wide[1] * a1 + wide[2] * a2)
        r_out[i] = a0 - (wide[0] * a1 + wide[1] * a2 + wide[2] * y3[i])


def kernel(fn, outs, scratch=(), flops=0, flagged=False, scalars=False, fetched=0, limit=24):
    def call(*args):
        specs = [VMEM] * len(args)
        out_specs = [VMEM] * len(outs)
        if flagged:
            specs[0] = pl.BlockSpec(memory_space=pltpu.SMEM)
        if fetched:
            specs[-fetched:] = [pl.BlockSpec(memory_space=pltpu.HBM)] * fetched
        if scalars:
            out_specs[-1] = pl.BlockSpec(memory_space=pltpu.SMEM)
        return pl.pallas_call(
            fn,
            out_shape=[jax.ShapeDtypeStruct(s, F32) for s in outs],
            in_specs=specs,
            out_specs=out_specs,
            scratch_shapes=[pltpu.VMEM(s, F32) for s in scratch]
            + [pltpu.SemaphoreType.DMA((fetched,))] * bool(fetched),
            cost_estimate=pl.CostEstimate(
                flops=flops, bytes_accessed=flops // 8 + 1024, transcendentals=0
            ),
            compiler_params=pltpu.CompilerParams(vmem_limit_bytes=limit << 20),
        )(*args)

    return call


def send(x, pairs):
    return lax.ppermute(x, ALL, pairs)


def extended(flags, right_side, kappa_sq):
    _, cols, lanes = right_side.shape
    shape = lambda n: (n, cols, lanes)
    own, p0, p1, p2, p3, low2, high2 = kernel(
        start_kernel,
        [shape(8)] + [shape(2)] * 4 + [shape(3)] * 2,
        [right_side.shape] * 2,
        flops=10**6,
        flagged=True,
        fetched=2,
    )(flags, right_side, kappa_sq)
    relayed = [send(piece, spread) for piece, (spread, _) in zip((p0, p1, p2, high2), ROUTES)]
    swapped = [
        send(x, pairs)
        for x, pairs in ((own, EVEN), (own, ODD), (low2, LOW2), (high2, HIGH2), (high2, ACROSS))
    ]
    *pieces, ahead = [send(x, onward) for x, (_, onward) in zip(relayed, ROUTES)]
    pieces.append(send(p3, STEP))
    edge = (len(WIDE), 8, lanes)
    return kernel(
        gather_kernel, [shape(len(PLANES)), edge, edge], flops=10**6, flagged=True
    )(flags, own, *swapped, ahead, *pieces)


def steps(right_side, kappa_sq):
    cells = right_side.size * NGX * RANKS
    flags = place_flags()
    center, to_even, to_odd = extended(flags, right_side, kappa_sq)
    even = send(to_even, GY_EVEN)
    odd = send(to_odd, GY_ODD)
    block, wide = right_side.shape, (80, 256)
    n_plane, n_column = lax.axis_size(PLANE), lax.axis_size(COLUMN)
    counts = (16, 14, 14, 12, 10, 8, 6, 12, 8)
    y1, y2, y3, sums = kernel(
        powers_kernel,
        [block] * 3 + [(n_plane, 128)],
        [(n, *wide) for n in counts] + [(128, 128)],
        flops=20_000_000,
        flagged=True,
    )(flags, right_side, center, even, odd)
    sums = lax.all_to_all(sums.reshape(n_plane, 1, 128), PLANE, 0, 0).reshape(n_plane, 128)
    (sums,) = kernel(add_kernel, [(n_column, 128)], flops=20000)(sums)
    sums = lax.all_to_all(sums.reshape(n_column, 1, 128), COLUMN, 0, 0).reshape(n_column, 128)
    return kernel(
        functools.partial(finish_kernel, cells), [block, block, (3,)], flops=2_000_000, scalars=True
    )(sums, right_side, kappa_sq, y1, y2, y3)


def solution(mesh):
    finer = Mesh(mesh.devices.reshape(3, 4, 8, 4, 2), ("gx_0", "gx_1", "gx_2", "gy_0", "gy_1"))
    in_specs = (P(GX, GY, None), P(GX, GY, None))
    out_specs = (P(GX, GY, None), P(GX, GY, None), P())
    return jax.shard_map(steps, mesh=finer, in_specs=in_specs, out_specs=out_specs, check_vma=False)
```

```python
import functools

import jax
import jax.numpy as jnp
from jax import lax
from jax.experimental import pallas as pl
from jax.experimental.pallas import tpu as pltpu
from jax.sharding import Mesh
from jax.sharding import PartitionSpec as P


GX = ("gx_0", "gx_1", "gx_2")
GY = ("gy_0", "gy_1")
ALL = GX + GY
PLANE = ("gx_1", "gx_2")
COLUMN = ("gx_0", "gy_0", "gy_1")
HI, XS, YS, RANKS = 3, 4, 8, 8
NGX = HI * XS * YS
SEG = XS * YS
VMEM = pl.BlockSpec(memory_space=pltpu.VMEM)
F32 = jnp.float32


def over_gx(moves):
    return [(a % NGX * RANKS + h, b % NGX * RANKS + h) for a, b in moves for h in range(RANKS)]


def corner(hi, x, y):
    return hi % HI * SEG + x % XS * YS + y % YS


def FIRST(k):
    return corner(k, 0, 0)


def LAST(k):
    return corner(k, XS - 1, YS - 1)


def SIDE_A(k):
    return corner(k, 0, YS - 1)


def SIDE_B(k):
    return corner(k, XS - 1, 0)


def NEAR_LAST(k):
    return corner(k, XS - 2, YS - 1)


def NEAR_FIRST(k):
    return corner(k, 1, 0)


SEGS = range(HI)
EVEN = over_gx([(g, g ^ 1) for g in range(NGX)])
ODD = over_gx([(g, ((g + 1) ^ 1) - 1) for g in range(NGX) if g % SEG not in (0, SEG - 1)])
STEP = over_gx(
    [(LAST(k), FIRST(k + 1)) for k in SEGS] + [(FIRST(k), LAST(k - 1)) for k in SEGS]
)
LOW2 = over_gx([(g, g ^ 2) for g in range(NGX)])
HIGH2 = over_gx([(g, ((g + 2) ^ 2) - 2) for g in range(NGX) if 1 < g % SEG < SEG - 2])
ACROSS = over_gx(
    [(LAST(k) - 1, FIRST(k + 1)) for k in SEGS] + [(FIRST(k) + 1, LAST(k - 1)) for k in SEGS]
)
ROUTES = [
    (
        over_gx([(LAST(k), SIDE_A(k)) for k in SEGS] + [(FIRST(k), SIDE_B(k)) for k in SEGS]),
        over_gx([(SIDE_A(k), FIRST(k + 1)) for k in SEGS] + [(SIDE_B(k), LAST(k - 1)) for k in SEGS]),
    ),
    (
        over_gx([(LAST(k), SIDE_B(k)) for k in SEGS] + [(FIRST(k), SIDE_A(k)) for k in SEGS]),
        over_gx([(SIDE_B(k), FIRST(k + 1)) for k in SEGS] + [(SIDE_A(k), LAST(k - 1)) for k in SEGS]),
    ),
    (
        over_gx([(LAST(k), NEAR_LAST(k)) for k in SEGS] + [(FIRST(k), NEAR_FIRST(k)) for k in SEGS]),
        over_gx([(NEAR_LAST(k), FIRST(k + 1)) for k in SEGS] + [(NEAR_FIRST(k), LAST(k - 1)) for k in SEGS]),
    ),
    (
        over_gx([(LAST(k), corner(k, XS - 1, 1)) for k in SEGS] + [(FIRST(k), corner(k, 0, YS - 2)) for k in SEGS]),
        over_gx(
            [(corner(k, XS - 1, 1), FIRST(k + 1) + 1) for k in SEGS]
            + [(corner(k, 0, YS - 2), LAST(k - 1) - 1) for k in SEGS]
        ),
    ),
]
GY_EVEN = [(g * RANKS + h, g * RANKS + (h ^ 1)) for g in range(NGX) for h in range(RANKS)]
GY_ODD = [
    (g * RANKS + h, g * RANKS + (((h + 1) ^ 1) - 1) % RANKS) for g in range(NGX) for h in range(RANKS)
]

ORDER = (("v", 0), ("v", 1), ("k", 0), ("k", 1), ("k", 2), ("v", 2), ("v", 3), ("k", 3))
AT = {what: i for i, what in enumerate(ORDER)}
PLANES = (
    [("pp", 0), ("pp", 1)]
    + [(name, AT["v", i]) for name in ("prev", "own", "next") for i in range(4)]
    + [("nn", 0), ("nn", 1), ("pp", 2)]
    + [(name, AT["k", i]) for name in ("prev", "own", "next") for i in range(4)]
    + [("nn", 2)]
)

WIDE = tuple(j for j in range(len(PLANES)) if j not in (0, 15, 16, 29))


def two_sum(a, b):
    s = a + b
    t = s - a
    return s, (a - (s - t)) + (b - t)


def quick(a, b):
    s = a + b
    return s, b - (s - a)


def halves(a):
    c = a * F32(4097.0)
    h = c - (c - a)
    return h, a - h


def two_prod(a, b):
    p = a * b
    (ah, al), (bh, bl) = halves(a), halves(b)
    return p, ((ah * bh - p) + ah * bl + al * bh) + al * bl


def add(a, b):
    s, e = two_sum(a[0], b[0])
    t, f = two_sum(a[1], b[1])
    s, e = quick(s, e + t)
    return quick(s, e + f)


def neg(a):
    return -a[0], -a[1]


def sub(a, b):
    return add(a, neg(b))


def mul(a, b):
    p, e = two_prod(a[0], b[0])
    return quick(p, e + (a[0] * b[1] + a[1] * b[0]))


def twice(a):
    return a[0] + a[0], a[1] + a[1]


def div(a, b):
    q = a[0] / b[0]
    r = sub(a, mul(b, (q, jnp.zeros_like(q))))
    return quick(q, r[0] / b[0])


def form(c, table):
    n = len(c)
    total = None
    for a in range(n):
        for b in range(a, n):
            t = table(a, b)
            for f in (c[a], c[b]):
                t = t if f is None else mul(t, f)
            t = t if a == b else twice(t)
            total = t if total is None else add(total, t)
    return total


def coefficients(mu, gram):
    hankel = lambda a, b: mu[a + b]
    lifted = lambda a, b: mu[a + b + 1]
    gamma = mu[0]
    alpha0 = div(gamma, mu[1])
    rr = [gram(0, 0)]
    r1 = [None, neg(alpha0)]
    gamma1 = form(r1, hankel)
    delta1 = form(r1, lifted)
    rr.append(form(r1, gram))
    beta1 = div(gamma1, gamma)
    alpha1 = div(gamma1, sub(delta1, div(mul(beta1, gamma1), alpha0)))
    one = (jnp.ones_like(alpha0[0]), jnp.zeros_like(alpha0[0]))
    p1 = [add(one, beta1), neg(alpha0)]
    step1 = [mul(alpha1, p1[0]), mul(alpha1, p1[1])]
    r2 = [None, sub(neg(alpha0), step1[0]), neg(step1[1])]
    gamma2 = form(r2, hankel)
    delta2 = form(r2, lifted)
    rr.append(form(r2, gram))
    beta2 = div(gamma2, gamma1)
    alpha2 = div(gamma2, sub(delta2, div(mul(beta2, gamma2), alpha1)))
    p2 = [add(one, mul(beta2, p1[0])), add(r2[1], mul(beta2, p1[1])), r2[2]]
    x = [
        add(add(alpha0, step1[0]), mul(alpha2, p2[0])),
        add(step1[1], mul(alpha2, p2[1])),
        mul(alpha2, p2[2]),
    ]
    return [c[0] for c in x], [c[0] for c in rr]


def around(src, i):
    c = src[i]
    rows, lanes = c.shape
    total = src[i - 1] + src[i + 1]
    total = total + pltpu.roll(c, 1, 0) + pltpu.roll(c, rows - 1, 0)
    return c, total + pltpu.roll(c, 1, 1) + pltpu.roll(c, lanes - 1, 1)


def lanes_of(shape):
    return lax.broadcasted_iota(jnp.int32, shape, len(shape) - 1)


def place_flags():
    place = lax.axis_index(PLANE)
    beside = (place == 0) | (place == SEG - 1)
    near = (place < 2) | (place >= SEG - 2)
    return jnp.stack(
        [place % 2 == 1, place % 4 >= 2, lax.axis_index("gy_1") == 1, beside, near]
    ).astype(jnp.int32)


def start_kernel(flags, rhs_hbm, kappa_hbm, own, p0, p1, p2, p3, low2, high2, rhs, kappa, sems):
    fetch = [
        pltpu.make_async_copy(rhs_hbm, rhs, sems.at[0]),
        pltpu.make_async_copy(kappa_hbm, kappa, sems.at[1]),
    ]
    for copy in fetch:
        copy.start()
    for copy in fetch:
        copy.wait()
    for i in range(4):
        k = kappa[i]
        shifted = 6.0 + k
        own[AT["v", i]] = (1.0 / (shifted * shifted + 6.0)) * rhs[i]
        own[AT["k", i]] = k
    for i, piece in enumerate((p0, p1, p2, p3)):
        piece[...] = own[2 * i : 2 * i + 2]

    @pl.when(flags[1] == 0)
    def _():
        low2[...] = own[5:8]
        high2[...] = own[0:3]

    @pl.when(flags[1] == 1)
    def _():
        low2[...] = own[0:3]
        high2[...] = own[5:8]


def gather_kernel(
    flags, own, even, odd, low2, high2, across, ahead, d0, d1, d2, d3, center, to_even, to_odd
):
    even_side = pl.multiple_of((1 - flags[2]) * 56, 8)
    odd_side = pl.multiple_of(flags[2] * 56, 8)

    def lay(part, ref):
        for j, (name, at) in enumerate(PLANES):
            if name == part:
                src, i = ((d0, d1, d2, d3)[at // 2], at % 2) if ref is None else (ref, at)
                center[j] = src[i]
                if j in WIDE:
                    to_even[WIDE.index(j)] = src[i, pl.ds(even_side, 8)]
                    to_odd[WIDE.index(j)] = src[i, pl.ds(odd_side, 8)]

    def when(*conditions):
        here = functools.reduce(lambda a, b: a & b, [flags[i] == value for i, value in conditions])
        return pl.when(here)

    lay("own", own)
    for value, (by_even, by_odd) in enumerate((("next", "prev"), ("prev", "next"))):

        @when((0, value))
        def _():
            lay(by_even, even)

        @when((0, value), (3, 0))
        def _():
            lay(by_odd, odd)

        @when((0, value), (3, 1))
        def _():
            lay(by_odd, None)

    for value, (by_low, by_high) in enumerate((("nn", "pp"), ("pp", "nn"))):

        @when((1, value))
        def _():
            lay(by_low, low2)

        @when((1, value), (4, 0))
        def _():
            lay(by_high, high2)

        @when((1, value), (3, 1))
        def _():
            lay(by_high, across)

        @when((1, value), (3, 0), (4, 1))
        def _():
            lay(by_high, ahead)


def powers(v, k, t1, w1, t2, w2, t3, y1s, y2s):
    def apply(src, dst, shift, count, scaled=None):
        for i in range(count):
            c, near = around(src, i + 1)
            kk = k[i + shift]
            y = kk * c - near
            dst[i] = y
            if scaled is not None:
                scaled[i] = (1.0 / (kk * kk + 6.0)) * y

    apply(v, t1, 0, 14)
    apply(t1, y1s, 1, 12, w1)
    apply(w1, t2, 2, 10)
    apply(t2, y2s, 3, 8, w2)
    apply(w2, t3, 4, 6)


def folded(a, b):
    prod = a * b
    prod = prod[:, :128] + prod[:, 128:]
    out = [prod[8 * j : 8 * j + 8] for j in range(prod.shape[0] // 8)]
    while len(out) > 1:
        out = [out[j] + out[j + 1] for j in range(0, len(out) - 1, 2)] + out[len(out) & ~1 :]
    return out[0]


def reduce_plane(i, cut, rhs, v, k, w1, w2, t3, y1s, y2s, outs, rows):
    c, near = around(t3, i + 1)
    y3 = cut(k[i + 5] * c - near)
    y0, y1, y2, g = rhs(i), cut(y1s[i + 4]), cut(y2s[i + 2]), cut(c)
    for out, y in zip(outs, (y1, y2, y3)):
        out[i] = y
    v0, v1, v2 = cut(v[i + 6]), cut(w1[i + 4]), cut(w2[i + 2])
    pairs = (
        (y0, v0), (y1, v0), (y1, v1), (y2, v1), (y2, v2), (g, g),
        (y0, y0), (y0, y1), (y0, y2), (y1, y1), (y1, y2), (y2, y2),
    )
    for d, (a, b) in enumerate(pairs):
        rows[8 * d : 8 * d + 8] += folded(a, b)


def inner_kernel(rhs, center, y1_out, y2_out, y3_out, rows, v, k, t1, w1, t2, w2, t3, y1s, y2s):
    for j in range(16):
        v[j] = center[j]
    for j in range(14):
        k[j] = 6.0 + center[j + 16]

    powers(v, k, t1, w1, t2, w2, t3, y1s, y2s)
    rows[...] = jnp.zeros_like(rows)

    for i in range(4):
        reduce_plane(
            i, lambda x: x[8:56], lambda p: rhs[p, 8:56], v, k, w1, w2, t3, y1s, y2s,
            (y1_out, y2_out, y3_out), rows,
        )


def outer_kernel(
    flags, rhs, center, even, odd, inner_rows,
    y1_out, y2_out, y3_out, sums_out,
    v, k, t1, w1, t2, w2, t3, y1s, y2s, rows,
):
    even_side = pl.multiple_of((1 - flags[2]) * 40, 8)
    odd_side = pl.multiple_of(flags[2] * 40, 8)
    for j in range(30):
        ref, at, base = (v, j, 0.0) if j < 16 else (k, j - 16, 6.0)
        put = lambda plane: plane if ref is v else base + plane
        ref[at, 8:24] = put(center[j, 0:16])
        ref[at, 24:40] = put(center[j, 48:64])
        if j in WIDE:
            ref[at, pl.ds(even_side, 8)] = put(even[WIDE.index(j)])
            ref[at, pl.ds(odd_side, 8)] = put(odd[WIDE.index(j)])
        else:
            ref[at, 0:8] = jnp.zeros((8, ref.shape[2]), F32)
            ref[at, 40:48] = jnp.zeros((8, ref.shape[2]), F32)

    powers(v, k, t1, w1, t2, w2, t3, y1s, y2s)
    rows[...] = inner_rows[...]
    ends = lambda x, a, b: jnp.concatenate([x[a : a + 8], x[b : b + 8]], axis=0)

    for i in range(4):
        reduce_plane(
            i, lambda x: ends(x, 8, 32), lambda p: ends(rhs[p], 0, 56), v, k, w1, w2, t3, y1s, y2s,
            (y1_out, y2_out, y3_out), rows,
        )

    terms = [rows[pl.ds(s, 16, stride=8), :] for s in range(8)]
    hi, lo = terms[0], jnp.zeros((16, 128), F32)
    for term in terms[1:]:
        hi, e = two_sum(hi, term)
        lo = lo + e
    for shift in (64, 32, 16, 8, 4, 2, 1):
        hi, e = two_sum(hi, pltpu.roll(hi, shift, 1))
        lo = lo + pltpu.roll(lo, shift, 1) + e
    row = lax.broadcasted_iota(jnp.int32, (16, 128), 0)
    lane = lanes_of((16, 128))
    packed = jnp.where(lane == row, hi, 0.0) + jnp.where(lane == row + 16, lo, 0.0)
    sums_out[...] = jnp.broadcast_to(jnp.sum(packed, axis=0, keepdims=True), sums_out.shape)


def added(parts):
    tiles = [parts[8 * j : 8 * j + 8] for j in range(parts.shape[0] // 8)]
    hi, lo = tiles[0], jnp.zeros((8, 128), F32)
    for tile in tiles[1:]:
        hi, e = two_sum(hi, tile)
        lo = lo + e
    for shift in (4, 2, 1):
        hi, e = two_sum(hi, pltpu.roll(hi, shift, 0))
        lo = lo + pltpu.roll(lo, shift, 0) + e
    lane = lanes_of((8, 128))
    return hi + jnp.where((lane >= 16) & (lane < 32), pltpu.roll(lo, 16, 1), 0.0)


def add_kernel(parts, out):
    out[...] = jnp.broadcast_to(added(parts[...])[0:1], out.shape)


def finish_kernel(cells, parts, rhs, kappa, i1, i2, i3, o1, o2, o3, x_out, r_out, rms_out):
    total = added(parts[...])[0:1]
    lane = lanes_of((1, 128))

    def pair(d):
        take = lambda i: jnp.sum(jnp.where(lane == i, total, 0.0), axis=1, keepdims=True)
        return take(d), take(d + 16)

    mu = [pair(d) for d in range(6)]
    table = [pair(6 + d) for d in range(6)]
    place = {(0, 0): 0, (0, 1): 1, (0, 2): 2, (1, 1): 3, (1, 2): 4, (2, 2): 5}
    c, rr = coefficients(mu, lambda a, b: table[place[a, b]])
    for i in range(3):
        rms_out[i] = jnp.sqrt(rr[i] / F32(cells))[0, 0]
    for i in range(4):
        for at, size, (y1, y2, y3), own in (
            (8, 48, (i1, i2, i3), 0), (0, 8, (o1, o2, o3), 0), (56, 8, (o1, o2, o3), 8)
        ):
            rows = slice(at, at + size)
            take = lambda ref: ref[i, own : own + size]
            a0, a1, a2, a3 = rhs[i, rows], take(y1), take(y2), take(y3)
            kk = 6.0 + kappa[i, rows]
            x_out[i, rows] = (1.0 / (kk * kk + 6.0)) * (c[0] * a0 + c[1] * a1 + c[2] * a2)
            r_out[i, rows] = a0 - (c[0] * a1 + c[1] * a2 + c[2] * a3)


def kernel(fn, outs, scratch=(), flops=0, flagged=False, scalars=False, fetched=0, limit=24):
    def call(*args):
        specs = [VMEM] * len(args)
        out_specs = [VMEM] * len(outs)
        if flagged:
            specs[0] = pl.BlockSpec(memory_space=pltpu.SMEM)
        if fetched:
            specs[-fetched:] = [pl.BlockSpec(memory_space=pltpu.HBM)] * fetched
        if scalars:
            out_specs[-1] = pl.BlockSpec(memory_space=pltpu.SMEM)
        return pl.pallas_call(
            fn,
            out_shape=[jax.ShapeDtypeStruct(s, F32) for s in outs],
            in_specs=specs,
            out_specs=out_specs,
            scratch_shapes=[pltpu.VMEM(s, F32) for s in scratch]
            + [pltpu.SemaphoreType.DMA((fetched,))] * bool(fetched),
            cost_estimate=pl.CostEstimate(
                flops=flops, bytes_accessed=flops // 8 + 1024, transcendentals=0
            ),
            compiler_params=pltpu.CompilerParams(vmem_limit_bytes=limit << 20),
        )(*args)

    return call


def send(x, pairs):
    return lax.ppermute(x, ALL, pairs)


def extended(flags, right_side, kappa_sq):
    _, cols, lanes = right_side.shape
    shape = lambda n: (n, cols, lanes)
    own, p0, p1, p2, p3, low2, high2 = kernel(
        start_kernel,
        [shape(8)] + [shape(2)] * 4 + [shape(3)] * 2,
        [right_side.shape] * 2,
        flops=10**6,
        flagged=True,
        fetched=2,
    )(flags, right_side, kappa_sq)
    relayed = [send(piece, spread) for piece, (spread, _) in zip((p0, p1, p2, high2), ROUTES)]
    swapped = [
        send(x, pairs)
        for x, pairs in ((own, EVEN), (own, ODD), (low2, LOW2), (high2, HIGH2), (high2, ACROSS))
    ]
    *pieces, ahead = [send(x, onward) for x, (_, onward) in zip(relayed, ROUTES)]
    pieces.append(send(p3, STEP))
    edge = (len(WIDE), 8, lanes)
    return kernel(
        gather_kernel, [shape(len(PLANES)), edge, edge], flops=10**6, flagged=True
    )(flags, own, *swapped, ahead, *pieces)


def steps(right_side, kappa_sq):
    cells = right_side.size * NGX * RANKS
    flags = place_flags()
    center, to_even, to_odd = extended(flags, right_side, kappa_sq)
    even = send(to_even, GY_EVEN)
    odd = send(to_odd, GY_ODD)
    block, lanes = right_side.shape, right_side.shape[2]
    n_plane, n_column = lax.axis_size(PLANE), lax.axis_size(COLUMN)
    counts = (16, 14, 14, 12, 10, 8, 6, 12, 8)
    *inner, rows = kernel(
        inner_kernel,
        [(4, 48, lanes)] * 3 + [(128, 128)],
        [(n, 64, lanes) for n in counts],
        flops=20_000_000,
    )(right_side, center)
    *outer, sums = kernel(
        outer_kernel,
        [(4, 16, lanes)] * 3 + [(n_plane, 128)],
        [(n, 48, lanes) for n in counts] + [(128, 128)],
        flops=12_000_000,
        flagged=True,
    )(flags, right_side, center, even, odd, rows)
    sums = lax.all_to_all(sums.reshape(n_plane, 1, 128), PLANE, 0, 0).reshape(n_plane, 128)
    (sums,) = kernel(add_kernel, [(n_column, 128)], flops=20000)(sums)
    sums = lax.all_to_all(sums.reshape(n_column, 1, 128), COLUMN, 0, 0).reshape(n_column, 128)
    return kernel(
        functools.partial(finish_kernel, cells), [block, block, (3,)], flops=2_000_000, scalars=True
    )(sums, right_side, kappa_sq, *inner, *outer)


def solution(mesh):
    finer = Mesh(mesh.devices.reshape(3, 4, 8, 4, 2), ("gx_0", "gx_1", "gx_2", "gy_0", "gy_1"))
    in_specs = (P(GX, GY, None), P(GX, GY, None))
    out_specs = (P(GX, GY, None), P(GX, GY, None), P())
    return jax.shard_map(steps, mesh=finer, in_specs=in_specs, out_specs=out_specs, check_vma=False)
```

```python
import functools

import jax
import jax.numpy as jnp
from jax import lax
from jax.experimental import pallas as pl
from jax.experimental.pallas import tpu as pltpu
from jax.sharding import Mesh
from jax.sharding import PartitionSpec as P


GX = ("gx_0", "gx_1", "gx_2")
GY = ("gy_0", "gy_1")
ALL = GX + GY
PLANE = ("gx_1", "gx_2")
COLUMN = ("gx_0", "gy_0", "gy_1")
HI, XS, YS, RANKS = 3, 4, 8, 8
NGX = HI * XS * YS
SEG = XS * YS
VMEM = pl.BlockSpec(memory_space=pltpu.VMEM)
F32 = jnp.float32


def over_gx(moves):
    return [(a % NGX * RANKS + h, b % NGX * RANKS + h) for a, b in moves for h in range(RANKS)]


def corner(hi, x, y):
    return hi % HI * SEG + x % XS * YS + y % YS


def FIRST(k):
    return corner(k, 0, 0)


def LAST(k):
    return corner(k, XS - 1, YS - 1)


def SIDE_A(k):
    return corner(k, 0, YS - 1)


def SIDE_B(k):
    return corner(k, XS - 1, 0)


def NEAR_LAST(k):
    return corner(k, XS - 2, YS - 1)


def NEAR_FIRST(k):
    return corner(k, 1, 0)


SEGS = range(HI)
EVEN = over_gx([(g, g ^ 1) for g in range(NGX)])
ODD = over_gx([(g, ((g + 1) ^ 1) - 1) for g in range(NGX) if g % SEG not in (0, SEG - 1)])
STEP = over_gx(
    [(LAST(k), FIRST(k + 1)) for k in SEGS] + [(FIRST(k), LAST(k - 1)) for k in SEGS]
)
LOW2 = over_gx([(g, g ^ 2) for g in range(NGX)])
HIGH2 = over_gx([(g, ((g + 2) ^ 2) - 2) for g in range(NGX) if 1 < g % SEG < SEG - 2])
ACROSS = over_gx(
    [(LAST(k) - 1, FIRST(k + 1)) for k in SEGS] + [(FIRST(k) + 1, LAST(k - 1)) for k in SEGS]
)
ROUTES = [
    (
        over_gx([(LAST(k), SIDE_A(k)) for k in SEGS] + [(FIRST(k), SIDE_B(k)) for k in SEGS]),
        over_gx([(SIDE_A(k), FIRST(k + 1)) for k in SEGS] + [(SIDE_B(k), LAST(k - 1)) for k in SEGS]),
    ),
    (
        over_gx([(LAST(k), SIDE_B(k)) for k in SEGS] + [(FIRST(k), SIDE_A(k)) for k in SEGS]),
        over_gx([(SIDE_B(k), FIRST(k + 1)) for k in SEGS] + [(SIDE_A(k), LAST(k - 1)) for k in SEGS]),
    ),
    (
        over_gx([(LAST(k), NEAR_LAST(k)) for k in SEGS] + [(FIRST(k), NEAR_FIRST(k)) for k in SEGS]),
        over_gx([(NEAR_LAST(k), FIRST(k + 1)) for k in SEGS] + [(NEAR_FIRST(k), LAST(k - 1)) for k in SEGS]),
    ),
    (
        over_gx([(LAST(k), corner(k, 1, YS - 1)) for k in SEGS] + [(FIRST(k), corner(k, 2, 0)) for k in SEGS]),
        over_gx(
            [(corner(k, 1, YS - 1), FIRST(k + 1) + 1) for k in SEGS]
            + [(corner(k, 2, 0), LAST(k - 1) - 1) for k in SEGS]
        ),
    ),
]
GY_EVEN = [(g * RANKS + h, g * RANKS + (h ^ 1)) for g in range(NGX) for h in range(RANKS)]
GY_ODD = [
    (g * RANKS + h, g * RANKS + (((h + 1) ^ 1) - 1) % RANKS) for g in range(NGX) for h in range(RANKS)
]

ORDER = (("v", 0), ("v", 1), ("k", 0), ("k", 1), ("k", 2), ("v", 2), ("v", 3), ("k", 3))
AT = {what: i for i, what in enumerate(ORDER)}
PLANES = (
    [("pp", 0), ("pp", 1)]
    + [(name, AT["v", i]) for name in ("prev", "own", "next") for i in range(4)]
    + [("nn", 0), ("nn", 1), ("pp", 2)]
    + [(name, AT["k", i]) for name in ("prev", "own", "next") for i in range(4)]
    + [("nn", 2)]
)

WHOLE = (5, 6, 7, 8, 9, 10) + (21, 22, 23, 24)
HALVES = ((1, 2), (3, 4), (11, 12), (13, 14), (17, 18), (19, 20), (25, 26), (27, 28))
TILES = len(WHOLE) + len(HALVES)
NONE = tuple(j for j in range(len(PLANES)) if j not in WHOLE + sum(HALVES, ()))


def two_sum(a, b):
    s = a + b
    t = s - a
    return s, (a - (s - t)) + (b - t)


def quick(a, b):
    s = a + b
    return s, b - (s - a)


def halves(a):
    c = a * F32(4097.0)
    h = c - (c - a)
    return h, a - h


def two_prod(a, b):
    p = a * b
    (ah, al), (bh, bl) = halves(a), halves(b)
    return p, ((ah * bh - p) + ah * bl + al * bh) + al * bl


def add(a, b):
    s, e = two_sum(a[0], b[0])
    t, f = two_sum(a[1], b[1])
    s, e = quick(s, e + t)
    return quick(s, e + f)


def neg(a):
    return -a[0], -a[1]


def sub(a, b):
    return add(a, neg(b))


def mul(a, b):
    p, e = two_prod(a[0], b[0])
    return quick(p, e + (a[0] * b[1] + a[1] * b[0]))


def twice(a):
    return a[0] + a[0], a[1] + a[1]


def div(a, b):
    q = a[0] / b[0]
    r = sub(a, mul(b, (q, jnp.zeros_like(q))))
    return quick(q, r[0] / b[0])


def form(c, table):
    n = len(c)
    total = None
    for a in range(n):
        for b in range(a, n):
            t = table(a, b)
            for f in (c[a], c[b]):
                t = t if f is None else mul(t, f)
            t = t if a == b else twice(t)
            total = t if total is None else add(total, t)
    return total


def coefficients(mu, gram):
    hankel = lambda a, b: mu[a + b]
    lifted = lambda a, b: mu[a + b + 1]
    gamma = mu[0]
    alpha0 = div(gamma, mu[1])
    rr = [gram(0, 0)]
    r1 = [None, neg(alpha0)]
    gamma1 = form(r1, hankel)
    delta1 = form(r1, lifted)
    rr.append(form(r1, gram))
    beta1 = div(gamma1, gamma)
    alpha1 = div(gamma1, sub(delta1, div(mul(beta1, gamma1), alpha0)))
    one = (jnp.ones_like(alpha0[0]), jnp.zeros_like(alpha0[0]))
    p1 = [add(one, beta1), neg(alpha0)]
    step1 = [mul(alpha1, p1[0]), mul(alpha1, p1[1])]
    r2 = [None, sub(neg(alpha0), step1[0]), neg(step1[1])]
    gamma2 = form(r2, hankel)
    delta2 = form(r2, lifted)
    rr.append(form(r2, gram))
    beta2 = div(gamma2, gamma1)
    alpha2 = div(gamma2, sub(delta2, div(mul(beta2, gamma2), alpha1)))
    p2 = [add(one, mul(beta2, p1[0])), add(r2[1], mul(beta2, p1[1])), r2[2]]
    x = [
        add(add(alpha0, step1[0]), mul(alpha2, p2[0])),
        add(step1[1], mul(alpha2, p2[1])),
        mul(alpha2, p2[2]),
    ]
    return [c[0] for c in x], [c[0] for c in rr]


def around(src, i):
    c = src[i]
    rows, lanes = c.shape
    total = src[i - 1] + src[i + 1]
    total = total + pltpu.roll(c, 1, 0) + pltpu.roll(c, rows - 1, 0)
    return c, total + pltpu.roll(c, 1, 1) + pltpu.roll(c, lanes - 1, 1)


def lanes_of(shape):
    return lax.broadcasted_iota(jnp.int32, shape, len(shape) - 1)


def place_flags():
    place = lax.axis_index(PLANE)
    beside = (place == 0) | (place == SEG - 1)
    near = (place < 2) | (place >= SEG - 2)
    return jnp.stack(
        [place % 2 == 1, place % 4 >= 2, lax.axis_index("gy_1") == 1, beside, near]
    ).astype(jnp.int32)


def start_kernel(flags, rhs_hbm, kappa_hbm, own, p0, p1, p2, p3, low2, high2, rhs, kappa, sems):
    fetch = [
        pltpu.make_async_copy(rhs_hbm, rhs, sems.at[0]),
        pltpu.make_async_copy(kappa_hbm, kappa, sems.at[1]),
    ]
    for copy in fetch:
        copy.start()
    for copy in fetch:
        copy.wait()
    for i in range(4):
        k = kappa[i]
        shifted = 6.0 + k
        own[AT["v", i]] = (1.0 / (shifted * shifted + 6.0)) * rhs[i]
        own[AT["k", i]] = k
    for i, piece in enumerate((p0, p1, p2, p3)):
        piece[...] = own[2 * i : 2 * i + 2]

    @pl.when(flags[1] == 0)
    def _():
        low2[...] = own[5:8]
        high2[...] = own[0:3]

    @pl.when(flags[1] == 1)
    def _():
        low2[...] = own[0:3]
        high2[...] = own[5:8]


def gather_kernel(
    flags, own, even, odd, low2, high2, across, ahead, d0, d1, d2, d3, center, to_even, to_odd
):
    def lay(part, ref):
        for j, (name, at) in enumerate(PLANES):
            if name == part:
                src, i = ((d0, d1, d2, d3)[at // 2], at % 2) if ref is None else (ref, at)
                center[j] = src[i]

    def when(*conditions):
        here = functools.reduce(lambda a, b: a & b, [flags[i] == value for i, value in conditions])
        return pl.when(here)

    lay("own", own)
    for value, (by_even, by_odd) in enumerate((("next", "prev"), ("prev", "next"))):

        @when((0, value))
        def _():
            lay(by_even, even)

        @when((0, value), (3, 0))
        def _():
            lay(by_odd, odd)

        @when((0, value), (3, 1))
        def _():
            lay(by_odd, None)

    for value, (by_low, by_high) in enumerate((("nn", "pp"), ("pp", "nn"))):

        @when((1, value))
        def _():
            lay(by_low, low2)

        @when((1, value), (4, 0))
        def _():
            lay(by_high, high2)

        @when((1, value), (3, 1))
        def _():
            lay(by_high, across)

        @when((1, value), (3, 0), (4, 1))
        def _():
            lay(by_high, ahead)

    upper = lax.broadcasted_iota(jnp.int32, (8, center.shape[2]), 0) < 4
    for out, last in ((to_even, flags[2] == 0), (to_odd, flags[2] == 1)):
        columns = pl.ds(pl.multiple_of(jnp.where(last, 56, 0), 8), 8)
        for t, j in enumerate(WHOLE):
            out[t] = center[j, columns]
        for t, (a, b) in enumerate(HALVES):
            a, b = center[a, columns], center[b, columns]
            out[len(WHOLE) + t] = jnp.where(
                last,
                jnp.where(upper, pltpu.roll(a, 4, 0), b),
                jnp.where(upper, a, pltpu.roll(b, 4, 0)),
            )


def powers(v, k, t1, w1, t2, w2, t3, y1s, y2s):
    def apply(src, dst, shift, count, scaled=None):
        for i in range(count):
            c, near = around(src, i + 1)
            kk = k[i + shift]
            y = kk * c - near
            dst[i] = y
            if scaled is not None:
                scaled[i] = (1.0 / (kk * kk + 6.0)) * y

    apply(v, t1, 0, 14)
    apply(t1, y1s, 1, 12, w1)
    apply(w1, t2, 2, 10)
    apply(t2, y2s, 3, 8, w2)
    apply(w2, t3, 4, 6)


def folded(a, b):
    prod = a * b
    prod = prod[:, :128] + prod[:, 128:]
    out = [prod[8 * j : 8 * j + 8] for j in range(prod.shape[0] // 8)]
    while len(out) > 1:
        out = [out[j] + out[j + 1] for j in range(0, len(out) - 1, 2)] + out[len(out) & ~1 :]
    return out[0]


def reduce_plane(i, cut, rhs, v, k, w1, w2, t3, y1s, y2s, outs, rows):
    c, near = around(t3, i + 1)
    y3 = cut(k[i + 5] * c - near)
    y0, y1, y2, g = rhs(i), cut(y1s[i + 4]), cut(y2s[i + 2]), cut(c)
    for out, y in zip(outs, (y1, y2, y3)):
        out[i] = y
    v0, v1, v2 = cut(v[i + 6]), cut(w1[i + 4]), cut(w2[i + 2])
    pairs = (
        (y0, v0), (y1, v0), (y1, v1), (y2, v1), (y2, v2), (g, g),
        (y0, y0), (y0, y1), (y0, y2), (y1, y1), (y1, y2), (y2, y2),
    )
    for d, (a, b) in enumerate(pairs):
        rows[8 * d : 8 * d + 8] += folded(a, b)


def inner_kernel(rhs, center, y1_out, y2_out, y3_out, rows, v, k, t1, w1, t2, w2, t3, y1s, y2s):
    for j in range(16):
        v[j] = center[j]
    for j in range(14):
        k[j] = 6.0 + center[j + 16]

    powers(v, k, t1, w1, t2, w2, t3, y1s, y2s)
    rows[...] = jnp.zeros_like(rows)

    for i in range(4):
        reduce_plane(
            i, lambda x: x[8:56], lambda p: rhs[p, 8:56], v, k, w1, w2, t3, y1s, y2s,
            (y1_out, y2_out, y3_out), rows,
        )


def outer_kernel(
    flags, rhs, center, even, odd, inner_rows,
    y1_out, y2_out, y3_out, sums_out,
    v, k, t1, w1, t2, w2, t3, y1s, y2s, rows,
):
    def at(j):
        return (v, j, 0.0) if j < 16 else (k, j - 16, 6.0)

    for j in range(30):
        ref, i, base = at(j)
        ref[i, 8:24] = base + center[j, 0:16] if base else center[j, 0:16]
        ref[i, 24:40] = base + center[j, 48:64] if base else center[j, 48:64]
        if j in NONE:
            ref[i, 0:8] = jnp.zeros((8, ref.shape[2]), F32)
            ref[i, 40:48] = jnp.zeros((8, ref.shape[2]), F32)
    for tiles, above in ((even, flags[2] == 0), (odd, flags[2] == 1)):
        side = pl.ds(pl.multiple_of(jnp.where(above, 40, 0), 8), 8)
        for t, j in enumerate(WHOLE):
            ref, i, base = at(j)
            ref[i, side] = base + tiles[t]
        for t, (a, b) in enumerate(HALVES):
            tile = tiles[len(WHOLE) + t]
            turned = pltpu.roll(tile, 4, 0)
            for j, first in ((a, True), (b, False)):
                ref, i, base = at(j)
                ref[i, side] = base + jnp.where(above == first, tile, turned)

    powers(v, k, t1, w1, t2, w2, t3, y1s, y2s)
    rows[...] = inner_rows[...]
    ends = lambda x, a, b: jnp.concatenate([x[a : a + 8], x[b : b + 8]], axis=0)

    for i in range(4):
        reduce_plane(
            i, lambda x: ends(x, 8, 32), lambda p: ends(rhs[p], 0, 56), v, k, w1, w2, t3, y1s, y2s,
            (y1_out, y2_out, y3_out), rows,
        )

    terms = [rows[pl.ds(s, 16, stride=8), :] for s in range(8)]
    hi, lo = terms[0], jnp.zeros((16, 128), F32)
    for term in terms[1:]:
        hi, e = two_sum(hi, term)
        lo = lo + e
    for shift in (64, 32, 16, 8, 4, 2, 1):
        hi, e = two_sum(hi, pltpu.roll(hi, shift, 1))
        lo = lo + pltpu.roll(lo, shift, 1) + e
    row = lax.broadcasted_iota(jnp.int32, (16, 128), 0)
    lane = lanes_of((16, 128))
    packed = jnp.where(lane == row, hi, 0.0) + jnp.where(lane == row + 16, lo, 0.0)
    sums_out[...] = jnp.broadcast_to(jnp.sum(packed, axis=0, keepdims=True), sums_out.shape)


def added(parts):
    tiles = [parts[8 * j : 8 * j + 8] for j in range(parts.shape[0] // 8)]
    hi, lo = tiles[0], jnp.zeros((8, 128), F32)
    for tile in tiles[1:]:
        hi, e = two_sum(hi, tile)
        lo = lo + e
    for shift in (4, 2, 1):
        hi, e = two_sum(hi, pltpu.roll(hi, shift, 0))
        lo = lo + pltpu.roll(lo, shift, 0) + e
    lane = lanes_of((8, 128))
    return hi + jnp.where((lane >= 16) & (lane < 32), pltpu.roll(lo, 16, 1), 0.0)


def add_kernel(parts, out):
    out[...] = jnp.broadcast_to(added(parts[...])[0:1], out.shape)


def finish_kernel(cells, parts, rhs, kappa, i1, i2, i3, o1, o2, o3, x_out, r_out, rms_out):
    total = added(parts[...])[0:1]
    lane = lanes_of((1, 128))

    def pair(d):
        take = lambda i: jnp.sum(jnp.where(lane == i, total, 0.0), axis=1, keepdims=True)
        return take(d), take(d + 16)

    mu = [pair(d) for d in range(6)]
    table = [pair(6 + d) for d in range(6)]
    place = {(0, 0): 0, (0, 1): 1, (0, 2): 2, (1, 1): 3, (1, 2): 4, (2, 2): 5}
    c, rr = coefficients(mu, lambda a, b: table[place[a, b]])
    for i in range(3):
        rms_out[i] = jnp.sqrt(rr[i] / F32(cells))[0, 0]
    for i in range(4):
        for at, size, (y1, y2, y3), own in (
            (8, 48, (i1, i2, i3), 0), (0, 8, (o1, o2, o3), 0), (56, 8, (o1, o2, o3), 8)
        ):
            rows = slice(at, at + size)
            take = lambda ref: ref[i, own : own + size]
            a0, a1, a2, a3 = rhs[i, rows], take(y1), take(y2), take(y3)
            kk = 6.0 + kappa[i, rows]
            x_out[i, rows] = (1.0 / (kk * kk + 6.0)) * (c[0] * a0 + c[1] * a1 + c[2] * a2)
            r_out[i, rows] = a0 - (c[0] * a1 + c[1] * a2 + c[2] * a3)


def kernel(fn, outs, scratch=(), flops=0, flagged=False, scalars=False, fetched=0, limit=24):
    def call(*args):
        specs = [VMEM] * len(args)
        out_specs = [VMEM] * len(outs)
        if flagged:
            specs[0] = pl.BlockSpec(memory_space=pltpu.SMEM)
        if fetched:
            specs[-fetched:] = [pl.BlockSpec(memory_space=pltpu.HBM)] * fetched
        if scalars:
            out_specs[-1] = pl.BlockSpec(memory_space=pltpu.SMEM)
        return pl.pallas_call(
            fn,
            out_shape=[jax.ShapeDtypeStruct(s, F32) for s in outs],
            in_specs=specs,
            out_specs=out_specs,
            scratch_shapes=[pltpu.VMEM(s, F32) for s in scratch]
            + [pltpu.SemaphoreType.DMA((fetched,))] * bool(fetched),
            cost_estimate=pl.CostEstimate(
                flops=flops, bytes_accessed=flops // 8 + 1024, transcendentals=0
            ),
            compiler_params=pltpu.CompilerParams(vmem_limit_bytes=limit << 20),
        )(*args)

    return call


def send(x, pairs):
    return lax.ppermute(x, ALL, pairs)


def extended(flags, right_side, kappa_sq):
    _, cols, lanes = right_side.shape
    shape = lambda n: (n, cols, lanes)
    own, p0, p1, p2, p3, low2, high2 = kernel(
        start_kernel,
        [shape(8)] + [shape(2)] * 4 + [shape(3)] * 2,
        [right_side.shape] * 2,
        flops=10**6,
        flagged=True,
        fetched=2,
    )(flags, *[pltpu.with_memory_space_constraint(x, pltpu.HBM) for x in (right_side, kappa_sq)])
    relayed = [send(piece, spread) for piece, (spread, _) in zip((p0, p1, p2, high2), ROUTES)]
    swapped = [
        send(x, pairs)
        for x, pairs in ((own, EVEN), (own, ODD), (low2, LOW2), (high2, HIGH2), (high2, ACROSS))
    ]
    *pieces, ahead = [send(x, onward) for x, (_, onward) in zip(relayed, ROUTES)]
    pieces.append(send(p3, STEP))
    edge = (TILES, 8, lanes)
    return kernel(
        gather_kernel, [shape(len(PLANES)), edge, edge], flops=10**6, flagged=True
    )(flags, own, *swapped, ahead, *pieces)


def steps(right_side, kappa_sq):
    cells = right_side.size * NGX * RANKS
    flags = place_flags()
    center, to_even, to_odd = extended(flags, right_side, kappa_sq)
    even = send(to_even, GY_EVEN)
    odd = send(to_odd, GY_ODD)
    block, lanes = right_side.shape, right_side.shape[2]
    n_plane, n_column = lax.axis_size(PLANE), lax.axis_size(COLUMN)
    counts = (16, 14, 14, 12, 10, 8, 6, 12, 8)
    *inner, rows = kernel(
        inner_kernel,
        [(4, 48, lanes)] * 3 + [(128, 128)],
        [(n, 64, lanes) for n in counts],
        flops=20_000_000,
    )(right_side, center)
    *outer, sums = kernel(
        outer_kernel,
        [(4, 16, lanes)] * 3 + [(n_plane, 128)],
        [(n, 48, lanes) for n in counts] + [(128, 128)],
        flops=12_000_000,
        flagged=True,
    )(flags, right_side, center, even, odd, rows)
    sums = lax.all_to_all(sums.reshape(n_plane, 1, 128), PLANE, 0, 0).reshape(n_plane, 128)
    (sums,) = kernel(add_kernel, [(n_column, 128)], flops=20000)(sums)
    sums = lax.all_to_all(sums.reshape(n_column, 1, 128), COLUMN, 0, 0).reshape(n_column, 128)
    return kernel(
        functools.partial(finish_kernel, cells), [block, block, (3,)], flops=2_000_000, scalars=True
    )(sums, right_side, kappa_sq, *inner, *outer)


def solution(mesh):
    finer = Mesh(mesh.devices.reshape(3, 4, 8, 4, 2), ("gx_0", "gx_1", "gx_2", "gy_0", "gy_1"))
    in_specs = (P(GX, GY, None), P(GX, GY, None))
    out_specs = (P(GX, GY, None), P(GX, GY, None), P())
    return jax.shard_map(steps, mesh=finer, in_specs=in_specs, out_specs=out_specs, check_vma=False)
```

```python
import functools

import jax
import jax.numpy as jnp
from jax import lax
from jax.experimental import pallas as pl
from jax.experimental.pallas import tpu as pltpu
from jax.sharding import Mesh
from jax.sharding import PartitionSpec as P


GX = ("gx_0", "gx_1", "gx_2")
GY = ("gy_0", "gy_1")
ALL = GX + GY
PLANE = ("gx_1", "gx_2")
COLUMN = ("gx_0", "gy_0", "gy_1")
HI, XS, YS, RANKS = 3, 4, 8, 8
NGX = HI * XS * YS
SEG = XS * YS
VMEM = pl.BlockSpec(memory_space=pltpu.VMEM)
F32 = jnp.float32


def over_gx(moves, ranks=range(RANKS)):
    return [(a % NGX * RANKS + h, b % NGX * RANKS + h) for a, b in moves for h in ranks]


def corner(hi, x, y):
    return hi % HI * SEG + x % XS * YS + y % YS


def FIRST(k):
    return corner(k, 0, 0)


def LAST(k):
    return corner(k, XS - 1, YS - 1)


SEGS = range(HI)
EVEN = over_gx([(g, g ^ 1) for g in range(NGX)])
ODD = over_gx([(g, ((g + 1) ^ 1) - 1) for g in range(NGX) if g % SEG not in (0, SEG - 1)])
STEP = over_gx(
    [(LAST(k), FIRST(k + 1)) for k in SEGS] + [(FIRST(k), LAST(k - 1)) for k in SEGS]
)
LOW2 = over_gx([(g, g ^ 2) for g in range(NGX)])
HIGH2 = over_gx([(g, ((g + 2) ^ 2) - 2) for g in range(NGX) if 1 < g % SEG < SEG - 2])
ACROSS = over_gx(
    [(LAST(k) - 1, FIRST(k + 1)) for k in SEGS] + [(FIRST(k) + 1, LAST(k - 1)) for k in SEGS]
)
RELAYS = (
    ((0, YS - 1), (XS - 1, 0), (0, YS - 2), (1, YS - 1)),
    ((2, YS - 1), (1, 0), (2, YS - 2), (2, 2)),
)


def route(i, ends):
    spread, onward = [], []
    for core, relays in enumerate(RELAYS):
        ranks = range(core, RANKS, 2)
        x, y = relays[i]
        for k in SEGS:
            up, down = corner(k, x, y), corner(k, XS - 1 - x, YS - 1 - y)
            spread += over_gx([(LAST(k), up), (FIRST(k), down)], ranks)
            onward += over_gx([(up, FIRST(k + 1) + ends), (down, LAST(k - 1) - ends)], ranks)
    return spread, onward


ROUTES = [route(0, 0), route(1, 0), route(2, 0), route(3, 1)]
CUTS = ((0, 3), (3, 5), (5, 7), (7, 8))

GY_EVEN = [(g * RANKS + h, g * RANKS + (h ^ 1)) for g in range(NGX) for h in range(RANKS)]
GY_ODD = [
    (g * RANKS + h, g * RANKS + (((h + 1) ^ 1) - 1) % RANKS) for g in range(NGX) for h in range(RANKS)
]

ORDER = (("v", 0), ("v", 1), ("k", 0), ("k", 1), ("k", 2), ("v", 2), ("v", 3), ("k", 3))
AT = {what: i for i, what in enumerate(ORDER)}
PLANES = (
    [("pp", 0), ("pp", 1)]
    + [(name, AT["v", i]) for name in ("prev", "own", "next") for i in range(4)]
    + [("nn", 0), ("nn", 1), ("pp", 2)]
    + [(name, AT["k", i]) for name in ("prev", "own", "next") for i in range(4)]
    + [("nn", 2)]
)

WHOLE = (5, 6, 7, 8, 9, 10) + (21, 22, 23, 24)
HALVES = ((1, 2), (3, 4), (11, 12), (13, 14), (17, 18), (19, 20), (25, 26), (27, 28))
TILES = len(WHOLE) + len(HALVES)
NONE = tuple(j for j in range(len(PLANES)) if j not in WHOLE + sum(HALVES, ()))


def two_sum(a, b):
    s = a + b
    t = s - a
    return s, (a - (s - t)) + (b - t)


def quick(a, b):
    s = a + b
    return s, b - (s - a)


def halves(a):
    c = a * F32(4097.0)
    h = c - (c - a)
    return h, a - h


def two_prod(a, b):
    p = a * b
    (ah, al), (bh, bl) = halves(a), halves(b)
    return p, ((ah * bh - p) + ah * bl + al * bh) + al * bl


def add(a, b):
    s, e = two_sum(a[0], b[0])
    t, f = two_sum(a[1], b[1])
    s, e = quick(s, e + t)
    return quick(s, e + f)


def neg(a):
    return -a[0], -a[1]


def sub(a, b):
    return add(a, neg(b))


def mul(a, b):
    p, e = two_prod(a[0], b[0])
    return quick(p, e + (a[0] * b[1] + a[1] * b[0]))


def twice(a):
    return a[0] + a[0], a[1] + a[1]


def div(a, b):
    q = a[0] / b[0]
    r = sub(a, mul(b, (q, jnp.zeros_like(q))))
    return quick(q, r[0] / b[0])


def form(c, table):
    n = len(c)
    total = None
    for a in range(n):
        for b in range(a, n):
            t = table(a, b)
            for f in (c[a], c[b]):
                t = t if f is None else mul(t, f)
            t = t if a == b else twice(t)
            total = t if total is None else add(total, t)
    return total


def coefficients(mu, gram):
    hankel = lambda a, b: mu[a + b]
    lifted = lambda a, b: mu[a + b + 1]
    gamma = mu[0]
    alpha0 = div(gamma, mu[1])
    rr = [gram(0, 0)]
    r1 = [None, neg(alpha0)]
    gamma1 = form(r1, hankel)
    delta1 = form(r1, lifted)
    rr.append(form(r1, gram))
    beta1 = div(gamma1, gamma)
    alpha1 = div(gamma1, sub(delta1, div(mul(beta1, gamma1), alpha0)))
    one = (jnp.ones_like(alpha0[0]), jnp.zeros_like(alpha0[0]))
    p1 = [add(one, beta1), neg(alpha0)]
    step1 = [mul(alpha1, p1[0]), mul(alpha1, p1[1])]
    r2 = [None, sub(neg(alpha0), step1[0]), neg(step1[1])]
    gamma2 = form(r2, hankel)
    delta2 = form(r2, lifted)
    rr.append(form(r2, gram))
    beta2 = div(gamma2, gamma1)
    alpha2 = div(gamma2, sub(delta2, div(mul(beta2, gamma2), alpha1)))
    p2 = [add(one, mul(beta2, p1[0])), add(r2[1], mul(beta2, p1[1])), r2[2]]
    x = [
        add(add(alpha0, step1[0]), mul(alpha2, p2[0])),
        add(step1[1], mul(alpha2, p2[1])),
        mul(alpha2, p2[2]),
    ]
    return [c[0] for c in x], [c[0] for c in rr]


def around(src, i):
    c = src[i]
    rows, lanes = c.shape
    total = src[i - 1] + src[i + 1]
    total = total + pltpu.roll(c, 1, 0) + pltpu.roll(c, rows - 1, 0)
    return c, total + pltpu.roll(c, 1, 1) + pltpu.roll(c, lanes - 1, 1)


def lanes_of(shape):
    return lax.broadcasted_iota(jnp.int32, shape, len(shape) - 1)


def place_flags():
    place = lax.axis_index(PLANE)
    beside = (place == 0) | (place == SEG - 1)
    near = (place < 2) | (place >= SEG - 2)
    return jnp.stack(
        [place % 2 == 1, place % 4 >= 2, lax.axis_index("gy_1") == 1, beside, near]
    ).astype(jnp.int32)


def start_kernel(flags, rhs_hbm, kappa_hbm, own, p0, p1, p2, p3, low2, high2, rhs, kappa, sems):
    fetch = [
        pltpu.make_async_copy(rhs_hbm, rhs, sems.at[0]),
        pltpu.make_async_copy(kappa_hbm, kappa, sems.at[1]),
    ]
    for copy in fetch:
        copy.start()
    for copy in fetch:
        copy.wait()
    for i in range(4):
        k = kappa[i]
        shifted = 6.0 + k
        own[AT["v", i]] = (1.0 / (shifted * shifted + 6.0)) * rhs[i]
        own[AT["k", i]] = k
    for (a, b), piece in zip(CUTS, (p0, p1, p2, p3)):
        piece[...] = own[a:b]

    @pl.when(flags[1] == 0)
    def _():
        low2[...] = own[5:8]
        high2[...] = own[0:3]

    @pl.when(flags[1] == 1)
    def _():
        low2[...] = own[0:3]
        high2[...] = own[5:8]


def gather_kernel(
    flags, own, even, odd, low2, high2, across, ahead, d0, d1, d2, d3, center, to_even, to_odd
):
    cut = [(piece, i) for (a, b), piece in zip(CUTS, (d0, d1, d2, d3)) for i in range(b - a)]

    def lay(part, ref):
        for j, (name, at) in enumerate(PLANES):
            if name == part:
                src, i = cut[at] if ref is None else (ref, at)
                center[j] = src[i]

    def when(*conditions):
        here = functools.reduce(lambda a, b: a & b, [flags[i] == value for i, value in conditions])
        return pl.when(here)

    lay("own", own)
    for value, (by_even, by_odd) in enumerate((("next", "prev"), ("prev", "next"))):

        @when((0, value))
        def _():
            lay(by_even, even)

        @when((0, value), (3, 0))
        def _():
            lay(by_odd, odd)

        @when((0, value), (3, 1))
        def _():
            lay(by_odd, None)

    for value, (by_low, by_high) in enumerate((("nn", "pp"), ("pp", "nn"))):

        @when((1, value))
        def _():
            lay(by_low, low2)

        @when((1, value), (4, 0))
        def _():
            lay(by_high, high2)

        @when((1, value), (3, 1))
        def _():
            lay(by_high, across)

        @when((1, value), (3, 0), (4, 1))
        def _():
            lay(by_high, ahead)

    upper = lax.broadcasted_iota(jnp.int32, (8, center.shape[2]), 0) < 4
    for out, last in ((to_even, flags[2] == 0), (to_odd, flags[2] == 1)):
        columns = pl.ds(pl.multiple_of(jnp.where(last, 56, 0), 8), 8)
        for t, j in enumerate(WHOLE):
            out[t] = center[j, columns]
        for t, (a, b) in enumerate(HALVES):
            a, b = center[a, columns], center[b, columns]
            out[len(WHOLE) + t] = jnp.where(
                last,
                jnp.where(upper, pltpu.roll(a, 4, 0), b),
                jnp.where(upper, a, pltpu.roll(b, 4, 0)),
            )


def powers(v, k, t1, w1, t2, w2, t3, y1s, y2s):
    def apply(src, dst, shift, count, scaled=None):
        for i in range(count):
            c, near = around(src, i + 1)
            kk = k[i + shift]
            y = kk * c - near
            dst[i] = y
            if scaled is not None:
                scaled[i] = (1.0 / (kk * kk + 6.0)) * y

    apply(v, t1, 0, 14)
    apply(t1, y1s, 1, 12, w1)
    apply(w1, t2, 2, 10)
    apply(t2, y2s, 3, 8, w2)
    apply(w2, t3, 4, 6)


def folded(a, b):
    prod = a * b
    prod = prod[:, :128] + prod[:, 128:]
    out = [prod[8 * j : 8 * j + 8] for j in range(prod.shape[0] // 8)]
    while len(out) > 1:
        out = [out[j] + out[j + 1] for j in range(0, len(out) - 1, 2)] + out[len(out) & ~1 :]
    return out[0]


def reduce_plane(i, cut, rhs, v, k, w1, w2, t3, y1s, y2s, outs, rows):
    c, near = around(t3, i + 1)
    y3 = cut(k[i + 5] * c - near)
    y0, y1, y2, g = rhs(i), cut(y1s[i + 4]), cut(y2s[i + 2]), cut(c)
    for out, y in zip(outs, (y1, y2, y3)):
        out[i] = y
    v0, v1, v2 = cut(v[i + 6]), cut(w1[i + 4]), cut(w2[i + 2])
    pairs = (
        (y0, v0), (y1, v0), (y1, v1), (y2, v1), (y2, v2), (g, g),
        (y0, y0), (y0, y1), (y0, y2), (y1, y1), (y1, y2), (y2, y2),
    )
    for d, (a, b) in enumerate(pairs):
        rows[8 * d : 8 * d + 8] += folded(a, b)


def inner_kernel(rhs, center, y1_out, y2_out, y3_out, rows, v, k, t1, w1, t2, w2, t3, y1s, y2s):
    for j in range(16):
        v[j] = center[j]
    for j in range(14):
        k[j] = 6.0 + center[j + 16]

    powers(v, k, t1, w1, t2, w2, t3, y1s, y2s)
    rows[...] = jnp.zeros_like(rows)

    for i in range(4):
        reduce_plane(
            i, lambda x: x[8:56], lambda p: rhs[p, 8:56], v, k, w1, w2, t3, y1s, y2s,
            (y1_out, y2_out, y3_out), rows,
        )


def outer_kernel(
    flags, rhs, center, even, odd, inner_rows,
    y1_out, y2_out, y3_out, sums_out,
    v, k, t1, w1, t2, w2, t3, y1s, y2s, rows,
):
    def at(j):
        return (v, j, 0.0) if j < 16 else (k, j - 16, 6.0)

    for j in range(30):
        ref, i, base = at(j)
        ref[i, 8:24] = base + center[j, 0:16] if base else center[j, 0:16]
        ref[i, 24:40] = base + center[j, 48:64] if base else center[j, 48:64]
        if j in NONE:
            ref[i, 0:8] = jnp.zeros((8, ref.shape[2]), F32)
            ref[i, 40:48] = jnp.zeros((8, ref.shape[2]), F32)
    for tiles, above in ((even, flags[2] == 0), (odd, flags[2] == 1)):
        side = pl.ds(pl.multiple_of(jnp.where(above, 40, 0), 8), 8)
        for t, j in enumerate(WHOLE):
            ref, i, base = at(j)
            ref[i, side] = base + tiles[t]
        for t, (a, b) in enumerate(HALVES):
            tile = tiles[len(WHOLE) + t]
            turned = pltpu.roll(tile, 4, 0)
            for j, first in ((a, True), (b, False)):
                ref, i, base = at(j)
                ref[i, side] = base + jnp.where(above == first, tile, turned)

    powers(v, k, t1, w1, t2, w2, t3, y1s, y2s)
    rows[...] = inner_rows[...]
    ends = lambda x, a, b: jnp.concatenate([x[a : a + 8], x[b : b + 8]], axis=0)

    for i in range(4):
        reduce_plane(
            i, lambda x: ends(x, 8, 32), lambda p: ends(rhs[p], 0, 56), v, k, w1, w2, t3, y1s, y2s,
            (y1_out, y2_out, y3_out), rows,
        )

    terms = [rows[pl.ds(s, 16, stride=8), :] for s in range(8)]
    hi, lo = terms[0], jnp.zeros((16, 128), F32)
    for term in terms[1:]:
        hi, e = two_sum(hi, term)
        lo = lo + e
    for shift in (64, 32, 16, 8, 4, 2, 1):
        hi, e = two_sum(hi, pltpu.roll(hi, shift, 1))
        lo = lo + pltpu.roll(lo, shift, 1) + e
    row = lax.broadcasted_iota(jnp.int32, (16, 128), 0)
    lane = lanes_of((16, 128))
    packed = jnp.where(lane == row, hi, 0.0) + jnp.where(lane == row + 16, lo, 0.0)
    sums_out[...] = jnp.broadcast_to(jnp.sum(packed, axis=0, keepdims=True), sums_out.shape)


def added(parts):
    tiles = [parts[8 * j : 8 * j + 8] for j in range(parts.shape[0] // 8)]
    hi, lo = tiles[0], jnp.zeros((8, 128), F32)
    for tile in tiles[1:]:
        hi, e = two_sum(hi, tile)
        lo = lo + e
    for shift in (4, 2, 1):
        hi, e = two_sum(hi, pltpu.roll(hi, shift, 0))
        lo = lo + pltpu.roll(lo, shift, 0) + e
    lane = lanes_of((8, 128))
    return hi + jnp.where((lane >= 16) & (lane < 32), pltpu.roll(lo, 16, 1), 0.0)


def add_kernel(parts, out):
    out[...] = jnp.broadcast_to(added(parts[...])[0:1], out.shape)


def finish_kernel(cells, parts, rhs, kappa, i1, i2, i3, o1, o2, o3, x_out, r_out, rms_out):
    total = added(parts[...])[0:1]
    lane = lanes_of((1, 128))

    def pair(d):
        take = lambda i: jnp.sum(jnp.where(lane == i, total, 0.0), axis=1, keepdims=True)
        return take(d), take(d + 16)

    mu = [pair(d) for d in range(6)]
    table = [pair(6 + d) for d in range(6)]
    place = {(0, 0): 0, (0, 1): 1, (0, 2): 2, (1, 1): 3, (1, 2): 4, (2, 2): 5}
    c, rr = coefficients(mu, lambda a, b: table[place[a, b]])
    for i in range(3):
        rms_out[i] = jnp.sqrt(rr[i] / F32(cells))[0, 0]
    for i in range(4):
        for at, size, (y1, y2, y3), own in (
            (8, 48, (i1, i2, i3), 0), (0, 8, (o1, o2, o3), 0), (56, 8, (o1, o2, o3), 8)
        ):
            rows = slice(at, at + size)
            take = lambda ref: ref[i, own : own + size]
            a0, a1, a2, a3 = rhs[i, rows], take(y1), take(y2), take(y3)
            kk = 6.0 + kappa[i, rows]
            x_out[i, rows] = (1.0 / (kk * kk + 6.0)) * (c[0] * a0 + c[1] * a1 + c[2] * a2)
            r_out[i, rows] = a0 - (c[0] * a1 + c[1] * a2 + c[2] * a3)


def kernel(fn, outs, scratch=(), flops=0, flagged=False, scalars=False, fetched=0, limit=24):
    def call(*args):
        specs = [VMEM] * len(args)
        out_specs = [VMEM] * len(outs)
        if flagged:
            specs[0] = pl.BlockSpec(memory_space=pltpu.SMEM)
        if fetched:
            specs[-fetched:] = [pl.BlockSpec(memory_space=pltpu.HBM)] * fetched
        if scalars:
            out_specs[-1] = pl.BlockSpec(memory_space=pltpu.SMEM)
        return pl.pallas_call(
            fn,
            out_shape=[jax.ShapeDtypeStruct(s, F32) for s in outs],
            in_specs=specs,
            out_specs=out_specs,
            scratch_shapes=[pltpu.VMEM(s, F32) for s in scratch]
            + [pltpu.SemaphoreType.DMA((fetched,))] * bool(fetched),
            cost_estimate=pl.CostEstimate(
                flops=flops, bytes_accessed=flops // 8 + 1024, transcendentals=0
            ),
            compiler_params=pltpu.CompilerParams(vmem_limit_bytes=limit << 20),
        )(*args)

    return call


def send(x, pairs):
    return lax.ppermute(x, ALL, pairs)


def extended(flags, right_side, kappa_sq):
    _, cols, lanes = right_side.shape
    shape = lambda n: (n, cols, lanes)
    own, p0, p1, p2, p3, low2, high2 = kernel(
        start_kernel,
        [shape(8)] + [shape(b - a) for a, b in CUTS] + [shape(3)] * 2,
        [right_side.shape] * 2,
        flops=10**6,
        flagged=True,
        fetched=2,
    )(flags, *[pltpu.with_memory_space_constraint(x, pltpu.HBM) for x in (right_side, kappa_sq)])
    relayed = [send(piece, spread) for piece, (spread, _) in zip((p0, p1, p2, high2), ROUTES)]
    swapped = [
        send(x, pairs)
        for x, pairs in ((own, EVEN), (own, ODD), (low2, LOW2), (high2, HIGH2), (high2, ACROSS))
    ]
    *pieces, ahead = [send(x, onward) for x, (_, onward) in zip(relayed, ROUTES)]
    pieces.append(send(p3, STEP))
    edge = (TILES, 8, lanes)
    return kernel(
        gather_kernel, [shape(len(PLANES)), edge, edge], flops=10**6, flagged=True
    )(flags, own, *swapped, ahead, *pieces)


def steps(right_side, kappa_sq):
    cells = right_side.size * NGX * RANKS
    flags = place_flags()
    center, to_even, to_odd = extended(flags, right_side, kappa_sq)
    even = send(to_even, GY_EVEN)
    odd = send(to_odd, GY_ODD)
    block, lanes = right_side.shape, right_side.shape[2]
    n_plane, n_column = lax.axis_size(PLANE), lax.axis_size(COLUMN)
    counts = (16, 14, 14, 12, 10, 8, 6, 12, 8)
    *inner, rows = kernel(
        inner_kernel,
        [(4, 48, lanes)] * 3 + [(128, 128)],
        [(n, 64, lanes) for n in counts],
        flops=20_000_000,
    )(right_side, center)
    *outer, sums = kernel(
        outer_kernel,
        [(4, 16, lanes)] * 3 + [(n_plane, 128)],
        [(n, 48, lanes) for n in counts] + [(128, 128)],
        flops=12_000_000,
        flagged=True,
    )(flags, right_side, center, even, odd, rows)
    sums = lax.all_to_all(sums.reshape(n_plane, 1, 128), PLANE, 0, 0).reshape(n_plane, 128)
    (sums,) = kernel(add_kernel, [(n_column, 128)], flops=20000)(sums)
    sums = lax.all_to_all(sums.reshape(n_column, 1, 128), COLUMN, 0, 0).reshape(n_column, 128)
    return kernel(
        functools.partial(finish_kernel, cells), [block, block, (3,)], flops=2_000_000, scalars=True
    )(sums, right_side, kappa_sq, *inner, *outer)


def solution(mesh):
    finer = Mesh(mesh.devices.reshape(3, 4, 8, 4, 2), ("gx_0", "gx_1", "gx_2", "gy_0", "gy_1"))
    in_specs = (P(GX, GY, None), P(GX, GY, None))
    out_specs = (P(GX, GY, None), P(GX, GY, None), P())
    return jax.shard_map(steps, mesh=finer, in_specs=in_specs, out_specs=out_specs, check_vma=False)
```

```python
import functools

import jax
import jax.numpy as jnp
from jax import lax
from jax.experimental import pallas as pl
from jax.experimental.pallas import tpu as pltpu
from jax.sharding import Mesh
from jax.sharding import PartitionSpec as P


GX = ("gx_0", "gx_1", "gx_2")
GY = ("gy_0", "gy_1")
ALL = GX + GY
PLANE = ("gx_1", "gx_2")
COLUMN = ("gx_0", "gy_0", "gy_1")
HI, XS, YS, RANKS = 3, 4, 8, 8
NGX = HI * XS * YS
SEG = XS * YS
VMEM = pl.BlockSpec(memory_space=pltpu.VMEM)
F32 = jnp.float32


def over_gx(moves, ranks=range(RANKS)):
    return [(a % NGX * RANKS + h, b % NGX * RANKS + h) for a, b in moves for h in ranks]


def corner(hi, x, y):
    return hi % HI * SEG + x % XS * YS + y % YS


def FIRST(k):
    return corner(k, 0, 0)


def LAST(k):
    return corner(k, XS - 1, YS - 1)


SEGS = range(HI)
EVEN = over_gx([(g, g ^ 1) for g in range(NGX)])
ODD = over_gx([(g, ((g + 1) ^ 1) - 1) for g in range(NGX) if g % SEG not in (0, SEG - 1)])
LOW2 = over_gx([(g, g ^ 2) for g in range(NGX)])
HIGH2 = over_gx([(g, ((g + 2) ^ 2) - 2) for g in range(NGX) if 1 < g % SEG < SEG - 2])
ACROSS = over_gx(
    [(LAST(k) - 1, FIRST(k + 1)) for k in SEGS] + [(FIRST(k) + 1, LAST(k - 1)) for k in SEGS]
)
RELAYS = (
    ((0, YS - 1), (XS - 1, 0), (0, YS - 2), (1, YS - 1)),
    ((2, YS - 1), (1, 0), (2, YS - 2), (2, 2)),
)


def route(i, ends):
    spread, onward = [], []
    for core, relays in enumerate(RELAYS):
        ranks = range(core, RANKS, 2)
        x, y = relays[i]
        for k in SEGS:
            up, down = corner(k, x, y), corner(k, XS - 1 - x, YS - 1 - y)
            spread += over_gx([(LAST(k), up), (FIRST(k), down)], ranks)
            onward += over_gx([(up, FIRST(k + 1) + ends), (down, LAST(k - 1) - ends)], ranks)
    return spread, onward


ROUTES = [route(0, 0), route(1, 0), route(2, 0), route(3, 1)]
CUTS = ((0, 3), (3, 6), (6, 8))

GY_EVEN = [(g * RANKS + h, g * RANKS + (h ^ 1)) for g in range(NGX) for h in range(RANKS)]
GY_ODD = [
    (g * RANKS + h, g * RANKS + (((h + 1) ^ 1) - 1) % RANKS) for g in range(NGX) for h in range(RANKS)
]

ORDER = (("v", 0), ("v", 1), ("k", 0), ("k", 1), ("k", 2), ("v", 2), ("v", 3), ("k", 3))
AT = {what: i for i, what in enumerate(ORDER)}
PLANES = (
    [("pp", 1), ("pp", 0)]
    + [(name, AT["v", i]) for name in ("prev", "own", "next") for i in range(4)]
    + [("nn", 0), ("nn", 1), None]
    + [(name, AT["k", i]) for name in ("prev", "own", "next") for i in range(4)]
    + [None]
)

WHOLE = (5, 6, 7, 8, 9, 10) + (21, 22, 23, 24)
HALVES = ((1, 2), (3, 4), (11, 12), (13, 14), (17, 18), (19, 20), (25, 26), (27, 28))
TILES = len(WHOLE) + len(HALVES)
NONE = tuple(j for j in range(len(PLANES)) if j not in WHOLE + sum(HALVES, ()))


def two_sum(a, b):
    s = a + b
    t = s - a
    return s, (a - (s - t)) + (b - t)


def quick(a, b):
    s = a + b
    return s, b - (s - a)


def halves(a):
    c = a * F32(4097.0)
    h = c - (c - a)
    return h, a - h


def two_prod(a, b):
    p = a * b
    (ah, al), (bh, bl) = halves(a), halves(b)
    return p, ((ah * bh - p) + ah * bl + al * bh) + al * bl


def add(a, b):
    s, e = two_sum(a[0], b[0])
    t, f = two_sum(a[1], b[1])
    s, e = quick(s, e + t)
    return quick(s, e + f)


def neg(a):
    return -a[0], -a[1]


def sub(a, b):
    return add(a, neg(b))


def mul(a, b):
    p, e = two_prod(a[0], b[0])
    return quick(p, e + (a[0] * b[1] + a[1] * b[0]))


def twice(a):
    return a[0] + a[0], a[1] + a[1]


def div(a, b):
    q = a[0] / b[0]
    r = sub(a, mul(b, (q, jnp.zeros_like(q))))
    return quick(q, r[0] / b[0])


def form(c, table):
    n = len(c)
    total = None
    for a in range(n):
        for b in range(a, n):
            t = table(a, b)
            for f in (c[a], c[b]):
                t = t if f is None else mul(t, f)
            t = t if a == b else twice(t)
            total = t if total is None else add(total, t)
    return total


def coefficients(mu, gram):
    hankel = lambda a, b: mu[a + b]
    lifted = lambda a, b: mu[a + b + 1]
    gamma = mu[0]
    alpha0 = div(gamma, mu[1])
    rr = [gram(0, 0)]
    r1 = [None, neg(alpha0)]
    gamma1 = form(r1, hankel)
    delta1 = form(r1, lifted)
    rr.append(form(r1, gram))
    beta1 = div(gamma1, gamma)
    alpha1 = div(gamma1, sub(delta1, div(mul(beta1, gamma1), alpha0)))
    one = (jnp.ones_like(alpha0[0]), jnp.zeros_like(alpha0[0]))
    p1 = [add(one, beta1), neg(alpha0)]
    step1 = [mul(alpha1, p1[0]), mul(alpha1, p1[1])]
    r2 = [None, sub(neg(alpha0), step1[0]), neg(step1[1])]
    gamma2 = form(r2, hankel)
    delta2 = form(r2, lifted)
    rr.append(form(r2, gram))
    beta2 = div(gamma2, gamma1)
    alpha2 = div(gamma2, sub(delta2, div(mul(beta2, gamma2), alpha1)))
    p2 = [add(one, mul(beta2, p1[0])), add(r2[1], mul(beta2, p1[1])), r2[2]]
    x = [
        add(add(alpha0, step1[0]), mul(alpha2, p2[0])),
        add(step1[1], mul(alpha2, p2[1])),
        mul(alpha2, p2[2]),
    ]
    return [c[0] for c in x], [c[0] for c in rr]


def around(src, i):
    c = src[i]
    rows, lanes = c.shape
    total = src[i - 1] + src[i + 1]
    total = total + pltpu.roll(c, 1, 0) + pltpu.roll(c, rows - 1, 0)
    return c, total + pltpu.roll(c, 1, 1) + pltpu.roll(c, lanes - 1, 1)


def lanes_of(shape):
    return lax.broadcasted_iota(jnp.int32, shape, len(shape) - 1)


def place_flags():
    place = lax.axis_index(PLANE)
    beside = (place == 0) | (place == SEG - 1)
    near = (place < 2) | (place >= SEG - 2)
    return jnp.stack(
        [place % 2 == 1, place % 4 >= 2, lax.axis_index("gy_1") == 1, beside, near]
    ).astype(jnp.int32)


def start_kernel(flags, rhs_hbm, kappa_hbm, own, p0, p1, p2, low2, high2, rhs, kappa, sems):
    fetch = [
        [
            pltpu.make_async_copy(hbm.at[i], ref.at[i], sems.at[j, i])
            for j, (hbm, ref) in enumerate(((rhs_hbm, rhs), (kappa_hbm, kappa)))
        ]
        for i in range(4)
    ]
    for copies in fetch:
        for copy in copies:
            copy.start()
    for i in range(4):
        for copy in fetch[i]:
            copy.wait()
        k = kappa[i]
        shifted = 6.0 + k
        own[AT["v", i]] = (1.0 / (shifted * shifted + 6.0)) * rhs[i]
        own[AT["k", i]] = k
    for (a, b), piece in zip(CUTS, (p0, p1, p2)):
        piece[...] = own[a:b]

    def near_side(out, near, beyond):
        c = own[AT["v", near]]
        rows, lanes = c.shape
        row = lax.broadcasted_iota(jnp.int32, c.shape, 0)
        total = own[AT["v", beyond]] + jnp.where(row > 0, pltpu.roll(c, 1, 0), 0.0)
        total = total + jnp.where(row < rows - 1, pltpu.roll(c, rows - 1, 0), 0.0)
        total = total + pltpu.roll(c, 1, 1) + pltpu.roll(c, lanes - 1, 1)
        out[0] = c
        out[1] = (6.0 + own[AT["k", near]]) * c - total

    @pl.when(flags[1] == 0)
    def _():
        near_side(low2, 3, 2)
        near_side(high2, 0, 1)

    @pl.when(flags[1] == 1)
    def _():
        near_side(low2, 0, 1)
        near_side(high2, 3, 2)


def gather_kernel(
    flags, own, even, odd, low2, high2, across, ahead, d0, d1, d2, center, to_even, to_odd
):
    cut = [(piece, i) for (a, b), piece in zip(CUTS, (d0, d1, d2)) for i in range(b - a)]

    def lay(part, ref):
        for j, plane in enumerate(PLANES):
            if plane and plane[0] == part:
                src, i = cut[plane[1]] if ref is None else (ref, plane[1])
                center[j] = src[i]

    def when(*conditions):
        here = functools.reduce(lambda a, b: a & b, [flags[i] == value for i, value in conditions])
        return pl.when(here)

    lay("own", own)
    for value, (by_even, by_odd) in enumerate((("next", "prev"), ("prev", "next"))):

        @when((0, value))
        def _():
            lay(by_even, even)

        @when((0, value), (3, 0))
        def _():
            lay(by_odd, odd)

        @when((0, value), (3, 1))
        def _():
            lay(by_odd, None)

    for value, (by_low, by_high) in enumerate((("nn", "pp"), ("pp", "nn"))):

        @when((1, value))
        def _():
            lay(by_low, low2)

        @when((1, value), (4, 0))
        def _():
            lay(by_high, high2)

        @when((1, value), (3, 1))
        def _():
            lay(by_high, across)

        @when((1, value), (3, 0), (4, 1))
        def _():
            lay(by_high, ahead)

    upper = lax.broadcasted_iota(jnp.int32, (8, center.shape[2]), 0) < 4
    for out, last in ((to_even, flags[2] == 0), (to_odd, flags[2] == 1)):
        columns = pl.ds(pl.multiple_of(jnp.where(last, 56, 0), 8), 8)
        for t, j in enumerate(WHOLE):
            out[t] = center[j, columns]
        for t, (a, b) in enumerate(HALVES):
            a, b = center[a, columns], center[b, columns]
            out[len(WHOLE) + t] = jnp.where(
                last,
                jnp.where(upper, pltpu.roll(a, 4, 0), b),
                jnp.where(upper, a, pltpu.roll(b, 4, 0)),
            )


def powers(v, k, t1, w1, t2, w2, t3, y1s, y2s, edges=None):
    def apply(src, dst, shift, count, scaled=None, first=0):
        for i in range(first, count):
            c, near = around(src, i + 1)
            kk = k[i + shift]
            y = kk * c - near
            dst[i] = y
            if scaled is not None:
                scaled[i] = (1.0 / (kk * kk + 6.0)) * y

    for i, partial, beside, own in ((0, 0, 2, 1), (13, 15, 13, 14)):
        t = v[partial] - v[beside]
        t1[i] = t if edges is None else t - edges(v[own])
    apply(v, t1, 0, 13, first=1)
    apply(t1, y1s, 1, 12, w1)
    apply(w1, t2, 2, 10)
    apply(t2, y2s, 3, 8, w2)
    apply(w2, t3, 4, 6)


def folded(a, b):
    prod = a * b
    prod = prod[:, :128] + prod[:, 128:]
    out = [prod[8 * j : 8 * j + 8] for j in range(prod.shape[0] // 8)]
    while len(out) > 1:
        out = [out[j] + out[j + 1] for j in range(0, len(out) - 1, 2)] + out[len(out) & ~1 :]
    return out[0]


def reduce_plane(i, cut, rhs, v, k, w1, w2, t3, y1s, y2s, outs, rows):
    c, near = around(t3, i + 1)
    y3 = cut(k[i + 5] * c - near)
    y0, y1, y2, g = rhs(i), cut(y1s[i + 4]), cut(y2s[i + 2]), cut(c)
    for out, y in zip(outs, (y1, y2, y3)):
        out[i] = y
    v0, v1, v2 = cut(v[i + 6]), cut(w1[i + 4]), cut(w2[i + 2])
    pairs = (
        (y0, v0), (y1, v0), (y1, v1), (y2, v1), (y2, v2), (g, g),
        (y0, y0), (y0, y1), (y0, y2), (y1, y1), (y1, y2), (y2, y2),
    )
    for d, (a, b) in enumerate(pairs):
        rows[8 * d : 8 * d + 8] += folded(a, b)


def inner_kernel(rhs, center, y1_out, y2_out, y3_out, rows, v, k, t1, w1, t2, w2, t3, y1s, y2s):
    for j in range(16):
        v[j] = center[j]
    for j in range(1, 13):
        k[j] = 6.0 + center[j + 16]

    powers(v, k, t1, w1, t2, w2, t3, y1s, y2s)
    rows[...] = jnp.zeros_like(rows)

    for i in range(4):
        reduce_plane(
            i, lambda x: x[8:56], lambda p: rhs[p, 8:56], v, k, w1, w2, t3, y1s, y2s,
            (y1_out, y2_out, y3_out), rows,
        )


def outer_kernel(
    flags, rhs, center, even, odd, inner_rows,
    y1_out, y2_out, y3_out, sums_out,
    v, k, t1, w1, t2, w2, t3, y1s, y2s, rows,
):
    def at(j):
        return (v, j, 0.0) if j < 16 else (k, j - 16, 6.0)

    for j in range(30):
        if PLANES[j] is None:
            continue
        ref, i, base = at(j)
        ref[i, 8:24] = base + center[j, 0:16] if base else center[j, 0:16]
        ref[i, 24:40] = base + center[j, 48:64] if base else center[j, 48:64]
        if j in NONE:
            ref[i, 0:8] = jnp.zeros((8, ref.shape[2]), F32)
            ref[i, 40:48] = jnp.zeros((8, ref.shape[2]), F32)
    for tiles, above in ((even, flags[2] == 0), (odd, flags[2] == 1)):
        side = pl.ds(pl.multiple_of(jnp.where(above, 40, 0), 8), 8)
        for t, j in enumerate(WHOLE):
            ref, i, base = at(j)
            ref[i, side] = base + tiles[t]
        for t, (a, b) in enumerate(HALVES):
            tile = tiles[len(WHOLE) + t]
            turned = pltpu.roll(tile, 4, 0)
            for j, first in ((a, True), (b, False)):
                ref, i, base = at(j)
                ref[i, side] = base + jnp.where(above == first, tile, turned)

    row = lax.broadcasted_iota(jnp.int32, v.shape[1:], 0)
    edges = lambda c: jnp.where(row == 8, pltpu.roll(c, 1, 0), 0.0) + jnp.where(
        row == 39, pltpu.roll(c, 47, 0), 0.0
    )
    powers(v, k, t1, w1, t2, w2, t3, y1s, y2s, edges)
    rows[...] = inner_rows[...]
    ends = lambda x, a, b: jnp.concatenate([x[a : a + 8], x[b : b + 8]], axis=0)

    for i in range(4):
        reduce_plane(
            i, lambda x: ends(x, 8, 32), lambda p: ends(rhs[p], 0, 56), v, k, w1, w2, t3, y1s, y2s,
            (y1_out, y2_out, y3_out), rows,
        )

    terms = [rows[pl.ds(s, 16, stride=8), :] for s in range(8)]
    hi, lo = terms[0], jnp.zeros((16, 128), F32)
    for term in terms[1:]:
        hi, e = two_sum(hi, term)
        lo = lo + e
    for shift in (64, 32, 16, 8, 4, 2, 1):
        hi, e = two_sum(hi, pltpu.roll(hi, shift, 1))
        lo = lo + pltpu.roll(lo, shift, 1) + e
    row = lax.broadcasted_iota(jnp.int32, (16, 128), 0)
    lane = lanes_of((16, 128))
    packed = jnp.where(lane == row, hi, 0.0) + jnp.where(lane == row + 16, lo, 0.0)
    sums_out[...] = jnp.broadcast_to(jnp.sum(packed, axis=0, keepdims=True), sums_out.shape)


def added(parts):
    tiles = [parts[8 * j : 8 * j + 8] for j in range(parts.shape[0] // 8)]
    hi, lo = tiles[0], jnp.zeros((8, 128), F32)
    for tile in tiles[1:]:
        hi, e = two_sum(hi, tile)
        lo = lo + e
    for shift in (4, 2, 1):
        hi, e = two_sum(hi, pltpu.roll(hi, shift, 0))
        lo = lo + pltpu.roll(lo, shift, 0) + e
    lane = lanes_of((8, 128))
    return hi + jnp.where((lane >= 16) & (lane < 32), pltpu.roll(lo, 16, 1), 0.0)


def add_kernel(parts, out):
    out[...] = jnp.broadcast_to(added(parts[...])[0:1], out.shape)


def finish_kernel(cells, parts, rhs, kappa, i1, i2, i3, o1, o2, o3, x_out, r_out, rms_out):
    total = added(parts[...])[0:1]
    lane = lanes_of((1, 128))

    def pair(d):
        take = lambda i: jnp.sum(jnp.where(lane == i, total, 0.0), axis=1, keepdims=True)
        return take(d), take(d + 16)

    mu = [pair(d) for d in range(6)]
    table = [pair(6 + d) for d in range(6)]
    place = {(0, 0): 0, (0, 1): 1, (0, 2): 2, (1, 1): 3, (1, 2): 4, (2, 2): 5}
    c, rr = coefficients(mu, lambda a, b: table[place[a, b]])
    for i in range(3):
        rms_out[i] = jnp.sqrt(rr[i] / F32(cells))[0, 0]
    for i in range(4):
        for at, size, (y1, y2, y3), own in (
            (8, 48, (i1, i2, i3), 0), (0, 8, (o1, o2, o3), 0), (56, 8, (o1, o2, o3), 8)
        ):
            rows = slice(at, at + size)
            take = lambda ref: ref[i, own : own + size]
            a0, a1, a2, a3 = rhs[i, rows], take(y1), take(y2), take(y3)
            kk = 6.0 + kappa[i, rows]
            x_out[i, rows] = (1.0 / (kk * kk + 6.0)) * (c[0] * a0 + c[1] * a1 + c[2] * a2)
            r_out[i, rows] = a0 - (c[0] * a1 + c[1] * a2 + c[2] * a3)


def kernel(fn, outs, scratch=(), flops=0, flagged=False, scalars=False, fetched=0, limit=24):
    def call(*args):
        specs = [VMEM] * len(args)
        out_specs = [VMEM] * len(outs)
        if flagged:
            specs[0] = pl.BlockSpec(memory_space=pltpu.SMEM)
        if fetched:
            specs[-fetched:] = [pl.BlockSpec(memory_space=pltpu.HBM)] * fetched
        if scalars:
            out_specs[-1] = pl.BlockSpec(memory_space=pltpu.SMEM)
        return pl.pallas_call(
            fn,
            out_shape=[jax.ShapeDtypeStruct(s, F32) for s in outs],
            in_specs=specs,
            out_specs=out_specs,
            scratch_shapes=[pltpu.VMEM(s, F32) for s in scratch]
            + [pltpu.SemaphoreType.DMA((fetched, 4))] * bool(fetched),
            cost_estimate=pl.CostEstimate(
                flops=flops, bytes_accessed=flops // 8 + 1024, transcendentals=0
            ),
            compiler_params=pltpu.CompilerParams(vmem_limit_bytes=limit << 20),
        )(*args)

    return call


def send(x, pairs):
    return lax.ppermute(x, ALL, pairs)


def extended(flags, right_side, kappa_sq):
    _, cols, lanes = right_side.shape
    shape = lambda n: (n, cols, lanes)
    own, p0, p1, p2, low2, high2 = kernel(
        start_kernel,
        [shape(8)] + [shape(b - a) for a, b in CUTS] + [shape(2)] * 2,
        [right_side.shape] * 2,
        flops=10**6,
        flagged=True,
        fetched=2,
    )(flags, *[pltpu.with_memory_space_constraint(x, pltpu.HBM) for x in (right_side, kappa_sq)])
    relayed = [send(piece, spread) for piece, (spread, _) in zip((p0, p1, p2, high2), ROUTES)]
    swapped = [
        send(x, pairs)
        for x, pairs in ((own, EVEN), (own, ODD), (low2, LOW2), (high2, HIGH2), (high2, ACROSS))
    ]
    *pieces, ahead = [send(x, onward) for x, (_, onward) in zip(relayed, ROUTES)]
    edge = (TILES, 8, lanes)
    return kernel(
        gather_kernel, [shape(len(PLANES)), edge, edge], flops=10**6, flagged=True
    )(flags, own, *swapped, ahead, *pieces)


def steps(right_side, kappa_sq):
    cells = right_side.size * NGX * RANKS
    flags = place_flags()
    center, to_even, to_odd = extended(flags, right_side, kappa_sq)
    even = send(to_even, GY_EVEN)
    odd = send(to_odd, GY_ODD)
    block, lanes = right_side.shape, right_side.shape[2]
    n_plane, n_column = lax.axis_size(PLANE), lax.axis_size(COLUMN)
    counts = (16, 14, 14, 12, 10, 8, 6, 12, 8)
    *inner, rows = kernel(
        inner_kernel,
        [(4, 48, lanes)] * 3 + [(128, 128)],
        [(n, 64, lanes) for n in counts],
        flops=20_000_000,
    )(right_side, center)
    *outer, sums = kernel(
        outer_kernel,
        [(4, 16, lanes)] * 3 + [(n_plane, 128)],
        [(n, 48, lanes) for n in counts] + [(128, 128)],
        flops=12_000_000,
        flagged=True,
    )(flags, right_side, center, even, odd, rows)
    sums = lax.all_to_all(sums.reshape(n_plane, 1, 128), PLANE, 0, 0).reshape(n_plane, 128)
    (sums,) = kernel(add_kernel, [(n_column, 128)], flops=20000)(sums)
    sums = lax.all_to_all(sums.reshape(n_column, 1, 128), COLUMN, 0, 0).reshape(n_column, 128)
    return kernel(
        functools.partial(finish_kernel, cells), [block, block, (3,)], flops=2_000_000, scalars=True
    )(sums, right_side, kappa_sq, *inner, *outer)


def solution(mesh):
    finer = Mesh(mesh.devices.reshape(3, 4, 8, 4, 2), ("gx_0", "gx_1", "gx_2", "gy_0", "gy_1"))
    in_specs = (P(GX, GY, None), P(GX, GY, None))
    out_specs = (P(GX, GY, None), P(GX, GY, None), P())
    return jax.shard_map(steps, mesh=finer, in_specs=in_specs, out_specs=out_specs, check_vma=False)
```
